8 devices in a mesh: dp: 2 (over z, y), gp: 4 (over x, core).
Axes of the slice: x: 2, y: 2, z: 1, core: 2. Of those that a mesh axis runs over, the one named last changes fastest.
Arguments:
- x_prev: float32 [32768, 83], P(('dp', 'gp')), parts along dimension 0
- x_cur: float32 [32768, 83], P(('dp', 'gp')), parts along dimension 0
- forcing: float32 [32768, 2, 5], P(('dp', 'gp')), parts along dimension 0
- grid_static: float32 [32768, 5], P(('dp', 'gp')), parts along dimension 0
- g2m_feat: float32 [32768, 4], P(('dp', 'gp')), parts along dimension 0
- m2g_feat: float32 [32768, 4], P(('dp', 'gp')), parts along dimension 0
- mesh_feat: float32 [8192, 3], P(('dp', 'gp')), parts along dimension 0
- mesh_edge_feat: float32 [8192, 6, 4], P(('dp', 'gp')), parts along dimension 0
- norm_stats: float32 [4, 83], replicated
- w_grid_in: bfloat16 [176, 512], replicated
- w_mesh_in: bfloat16 [3, 512], replicated
- w_eemb_in: bfloat16 [3, 4, 512], replicated
- w_embed_out: bfloat16 [5, 512, 512], replicated
- w_edge_in: bfloat16 [14, 1536, 512], replicated
- w_edge_out: bfloat16 [14, 512, 512], replicated
- w_node_in: bfloat16 [14, 1024, 512], replicated
- w_node_out: bfloat16 [14, 512, 512], replicated
- w_grid_self: bfloat16 [2, 512, 512], replicated
- w_out_hidden: bfloat16 [512, 512], replicated
- w_out_final: bfloat16 [512, 83], replicated
Outputs:
- output 1: float32 [32768, 83], P(('dp', 'gp')), parts along dimension 0
- output 2: float32 [32768, 83], P(('dp', 'gp')), parts along dimension 0
There are 2 independent parts. The reference program is written for one: setup_inputs(seed, part) draws one part's arguments, and reference() takes and returns one part's arrays. A program takes and returns all parts, laid end to end along the dimension named above; an argument that names none is the same for every part.
All inputs are finite; a program needn't handle non-finite values.
Results may differ from the reference program's by a relative error of at most 0.00789786.
Values are sent between devices in bfloat16 or wider.
A program may use at most 1 GiB of HBM per device.

```python
import jax
import jax.numpy as jnp
from jax import lax

GRID_NODES = 16384
MESH_NODES = 4096
SHIFT = 512
LATENT = 512
VARS = 83
FORCE = 5
STATIC = 5
LAYERS = 12
EDGE_FEAT = 4
MESH_FEAT = 3
OFFSET_COUNT = 6

GRID_RATIO = GRID_NODES // MESH_NODES
QUARTER = MESH_NODES // 4
BLOCKS = LAYERS + 2
IN_FEAT = 2 * VARS + FORCE + STATIC
OFFSETS = (1, -1, SHIFT, -SHIFT, QUARTER, -QUARTER)


def normal_weight(key_in, out_shape, fan_in):
    return (jax.random.normal(key_in, out_shape, jnp.float32) * fan_in ** -0.5).astype(jnp.bfloat16)


def setup_inputs(seed: int = 0, part: int = 0) -> dict:
    root_key = jax.random.key(seed)
    part_keys = jax.random.split(jax.random.fold_in(root_key, part), 8)
    weight_keys = jax.random.split(jax.random.key(seed + 1), 15)
    norm_stats = jnp.stack([
        0.5 * jax.random.normal(weight_keys[0], (VARS,), jnp.float32),
        jax.random.uniform(weight_keys[1], (VARS,), jnp.float32, 0.5, 1.5),
        0.2 * jax.random.normal(weight_keys[2], (VARS,), jnp.float32),
        jax.random.uniform(weight_keys[3], (VARS,), jnp.float32, 0.2, 0.6)])
    return {
        "x_prev": jax.random.normal(part_keys[0], (GRID_NODES, VARS), jnp.float32),
        "x_cur": jax.random.normal(part_keys[1], (GRID_NODES, VARS), jnp.float32),
        "forcing": jax.random.normal(part_keys[2], (GRID_NODES, 2, FORCE), jnp.float32),
        "grid_static": jax.random.normal(part_keys[3], (GRID_NODES, STATIC), jnp.float32),
        "g2m_feat": jax.random.normal(part_keys[4], (GRID_NODES, EDGE_FEAT), jnp.float32),
        "m2g_feat": jax.random.normal(part_keys[5], (GRID_NODES, EDGE_FEAT), jnp.float32),
        "mesh_feat": jax.random.normal(part_keys[6], (MESH_NODES, MESH_FEAT), jnp.float32),
        "mesh_edge_feat": jax.random.normal(part_keys[7], (MESH_NODES, OFFSET_COUNT, EDGE_FEAT), jnp.float32),
        "norm_stats": norm_stats,
        "w_grid_in": normal_weight(weight_keys[4], (IN_FEAT, LATENT), IN_FEAT),
        "w_mesh_in": normal_weight(weight_keys[5], (MESH_FEAT, LATENT), MESH_FEAT),
        "w_eemb_in": normal_weight(weight_keys[6], (3, EDGE_FEAT, LATENT), EDGE_FEAT),
        "w_embed_out": normal_weight(weight_keys[7], (5, LATENT, LATENT), LATENT),
        "w_edge_in": normal_weight(weight_keys[8], (BLOCKS, 3 * LATENT, LATENT), 3 * LATENT),
        "w_edge_out": normal_weight(weight_keys[9], (BLOCKS, LATENT, LATENT), LATENT),
        "w_node_in": normal_weight(weight_keys[10], (BLOCKS, 2 * LATENT, LATENT), 2 * LATENT),
        "w_node_out": normal_weight(weight_keys[11], (BLOCKS, LATENT, LATENT), LATENT),
        "w_grid_self": normal_weight(weight_keys[12], (2, LATENT, LATENT), LATENT),
        "w_out_hidden": normal_weight(weight_keys[13], (LATENT, LATENT), LATENT),
        "w_out_final": normal_weight(weight_keys[14], (LATENT, VARS), LATENT),
    }


def layer_norm(values):
    centre = jnp.mean(values, axis=-1, keepdims=True)
    centred = values - centre
    spread = jnp.mean(centred * centred, axis=-1, keepdims=True)
    return centred * lax.rsqrt(spread + 1e-5)


def matmul_f32(values, weight):
    return jnp.dot(values, weight, preferred_element_type=jnp.float32)


def mlp_tail(pre_act, w_second):
    hidden = jax.nn.silu(pre_act).astype(jnp.bfloat16)
    return layer_norm(matmul_f32(hidden, w_second))


def residual(base, update):
    return (base.astype(jnp.float32) + update).astype(jnp.bfloat16)


def embed_static(features, w_first, w_second):
    return mlp_tail(matmul_f32(features.astype(jnp.bfloat16), w_first), w_second).astype(jnp.bfloat16)


def reference(x_prev, x_cur, forcing, grid_static, g2m_feat, m2g_feat, mesh_feat, mesh_edge_feat, norm_stats, w_grid_in, w_mesh_in, w_eemb_in, w_embed_out, w_edge_in, w_edge_out, w_node_in, w_node_out, w_grid_self, w_out_hidden, w_out_final):
    mesh_lat = embed_static(mesh_feat, w_mesh_in, w_embed_out[1])
    g2m_lat = embed_static(g2m_feat, w_eemb_in[0], w_embed_out[2])
    m2g_lat = embed_static(m2g_feat, w_eemb_in[1], w_embed_out[3])
    edge_base = embed_static(mesh_edge_feat.reshape(MESH_NODES * OFFSET_COUNT, EDGE_FEAT), w_eemb_in[2], w_embed_out[4])
    in_mean = norm_stats[0]
    in_std = norm_stats[1]
    diff_mean = norm_stats[2]
    diff_std = norm_stats[3]

    def proc_layer(layer_state, layer_weights):
        mesh_cur, edge_lat = layer_state
        w_edge, w_edge_two, w_node, w_node_two = layer_weights
        send_proj = matmul_f32(mesh_cur, w_edge[LATENT:2 * LATENT])
        send_term = jnp.stack([jnp.roll(send_proj, -offset, axis=0) for offset in OFFSETS], axis=1).reshape(MESH_NODES * OFFSET_COUNT, LATENT)
        recv_term = matmul_f32(mesh_cur, w_edge[2 * LATENT:])
        pre_act = matmul_f32(edge_lat, w_edge[:LATENT]) + send_term
        pre_act = (pre_act.reshape(MESH_NODES, OFFSET_COUNT, LATENT) + recv_term[:, None, :]).reshape(MESH_NODES * OFFSET_COUNT, LATENT)
        edge_lat = residual(edge_lat, mlp_tail(pre_act, w_edge_two))
        edge_sum = jnp.sum(edge_lat.reshape(MESH_NODES, OFFSET_COUNT, LATENT).astype(jnp.float32), axis=1).astype(jnp.bfloat16)
        mesh_cur = residual(mesh_cur, mlp_tail(matmul_f32(mesh_cur, w_node[:LATENT]) + matmul_f32(edge_sum, w_node[LATENT:]), w_node_two))
        return (mesh_cur, edge_lat), None

    def forecast_step(state_pair, force_now):
        state_prev, state_cur = state_pair
        features = jnp.concatenate([(state_prev - in_mean) / in_std, (state_cur - in_mean) / in_std, force_now, grid_static], axis=1)
        grid_lat = embed_static(features, w_grid_in, w_embed_out[0])
        w_first = w_edge_in[0]
        senders = jnp.roll(grid_lat, SHIFT * GRID_RATIO, axis=0)
        recv_term = matmul_f32(mesh_lat, w_first[2 * LATENT:])
        pre_act = matmul_f32(g2m_lat, w_first[:LATENT]) + matmul_f32(senders, w_first[LATENT:2 * LATENT])
        pre_act = (pre_act.reshape(MESH_NODES, GRID_RATIO, LATENT) + recv_term[:, None, :]).reshape(GRID_NODES, LATENT)
        enc_edge = residual(g2m_lat, mlp_tail(pre_act, w_edge_out[0]))
        enc_sum = jnp.sum(enc_edge.reshape(MESH_NODES, GRID_RATIO, LATENT).astype(jnp.float32), axis=1).astype(jnp.bfloat16)
        node_first = w_node_in[0]
        mesh_cur = residual(mesh_lat, mlp_tail(matmul_f32(mesh_lat, node_first[:LATENT]) + matmul_f32(enc_sum, node_first[LATENT:]), w_node_out[0]))
        grid_cur = residual(grid_lat, mlp_tail(matmul_f32(grid_lat, w_grid_self[0]), w_grid_self[1]))
        layer_weights = (w_edge_in[1:BLOCKS - 1], w_edge_out[1:BLOCKS - 1], w_node_in[1:BLOCKS - 1], w_node_out[1:BLOCKS - 1])
        layer_out, no_stack = lax.scan(proc_layer, (mesh_cur, edge_base), layer_weights)
        mesh_cur = layer_out[0]
        w_last = w_edge_in[BLOCKS - 1]
        send_term = matmul_f32(jnp.roll(mesh_cur, -SHIFT, axis=0), w_last[LATENT:2 * LATENT])
        pre_act = matmul_f32(m2g_lat, w_last[:LATENT]) + matmul_f32(grid_cur, w_last[2 * LATENT:])
        pre_act = (pre_act.reshape(MESH_NODES, GRID_RATIO, LATENT) + send_term[:, None, :]).reshape(GRID_NODES, LATENT)
        dec_edge = residual(m2g_lat, mlp_tail(pre_act, w_edge_out[BLOCKS - 1]))
        node_last = w_node_in[BLOCKS - 1]
        grid_out = residual(grid_cur, mlp_tail(matmul_f32(grid_cur, node_last[:LATENT]) + matmul_f32(dec_edge, node_last[LATENT:]), w_node_out[BLOCKS - 1]))
        hidden = jax.nn.silu(matmul_f32(grid_out, w_out_hidden)).astype(jnp.bfloat16)
        prediction = matmul_f32(hidden, w_out_final)
        state_next = state_cur + diff_std * prediction + diff_mean
        return (state_cur, state_next), state_next

    final_pair, stacked = lax.scan(forecast_step, (x_prev, x_cur), jnp.swapaxes(forcing, 0, 1))
    return stacked[0], stacked[1]
```

```python
import functools

import jax
import jax.numpy as jnp
from jax import lax
from jax.experimental import pallas as pl
from jax.experimental.pallas import tpu as pltpu
from jax.sharding import PartitionSpec as P

F32 = jnp.float32
BF16 = jnp.bfloat16
LAT = 512
VARS = 83
LANES = 128
CELLS = 128
RATIO = 4
ROWS = CELLS * RATIO
SUB = 2
Q = 8
RLOC = 128
NODES = Q * RLOC
OFFS = 6
LAYERS = 12
TILE = 256
VMEM_LIMIT = 60 * 1024 * 1024


def mm(lhs, rhs):
    return jnp.dot(lhs, rhs, preferred_element_type=F32)


def silu(x):
    half = 0.5 * x
    return (half + half * jnp.tanh(half)).astype(BF16)


def norm(y):
    centred = y - jnp.sum(y, axis=-1, keepdims=True) * (1.0 / LAT)
    spread = jnp.sum(centred * centred, axis=-1, keepdims=True) * (1.0 / LAT)
    return centred * lax.rsqrt(spread + 1e-5)


def add_to(base, update):
    return (base.astype(F32) + update).astype(BF16)


def embed_kernel(x_ref, w_in_ref, w_out_ref, o_ref):
    o_ref[...] = norm(mm(silu(mm(x_ref[...], w_in_ref[0])), w_out_ref[0])).astype(BF16)


def embed_static(feats, w_in, w_out, starts, block=512):
    rows = feats.shape[0]

    def kind(i):
        return sum((i >= s // block).astype(jnp.int32) for s in starts)

    return pl.pallas_call(
        embed_kernel,
        grid=(rows // block,),
        in_specs=[
            pl.BlockSpec((block, LANES), lambda i: (i, 0)),
            pl.BlockSpec((1, LANES, LAT), lambda i: (kind(i), 0, 0)),
            pl.BlockSpec((1, LAT, LAT), lambda i: (kind(i), 0, 0)),
        ],
        out_specs=pl.BlockSpec((block, LAT), lambda i: (i, 0)),
        out_shape=jax.ShapeDtypeStruct((rows, LAT), BF16),
        compiler_params=pltpu.CompilerParams(vmem_limit_bytes=VMEM_LIMIT),
        name="embed",
    )(feats, w_in, w_out)


def by_member(ref, sub):
    return jnp.concatenate([ref[pl.ds(sub * ROWS + k, CELLS, stride=RATIO), :] for k in range(RATIO)], axis=0)


def tile4(x):
    return jnp.concatenate([x] * RATIO, axis=0)


def rows_of(sub, size):
    return pl.ds(sub * size, size)


def grid_kernel(names, decode, encode, *refs):
    r = dict(zip(names, refs))
    mean, std, diff_mean, diff_std = (r["stats"][i:i + 1, :] for i in range(4))
    lane = lax.broadcasted_iota(jnp.int32, (ROWS, LANES), 1)
    subs = range(SUB)
    cur = [by_member(r["cur"], s) for s in subs]
    if decode:
        grid_cur = [r["grid_cur"][rows_of(s, ROWS), :] for s in subs]
        pre = []
        for s in subs:
            send = mm(r["h_in"][s, 0], r["wl"][LAT:2 * LAT, :])
            both = mm(r["m2g"][rows_of(s, ROWS), :], r["wl"][:LAT, :]) + mm(grid_cur[s], r["wl"][2 * LAT:, :])
            pre.append(both + tile4(send))
        hid = [silu(p) for p in pre]
        upd = [mm(h, r["wl_out"][...]) for h in hid]
        edge = [add_to(r["m2g"][rows_of(s, ROWS), :], norm(upd[s])) for s in subs]
        pre = [mm(grid_cur[s], r["wl_node"][:LAT, :]) + mm(edge[s], r["wl_node"][LAT:, :]) for s in subs]
        hid = [silu(p) for p in pre]
        upd = [mm(h, r["wl_node_out"][...]) for h in hid]
        out = [add_to(grid_cur[s], norm(upd[s])) for s in subs]
        hid = [silu(mm(o, r["w_hidden"][...])) for o in out]
        pred = [mm(h, r["w_final"][...]) for h in hid]
        nxt = [cur[s] + diff_std * pred[s] + diff_mean for s in subs]
        for s in subs:
            for k in range(RATIO):
                r["next"][pl.ds(s * ROWS + k, CELLS, stride=RATIO), :] = nxt[s][k * CELLS:(k + 1) * CELLS, :VARS]
    if encode:
        if decode:
            first = cur
            second = [jnp.where(lane < VARS, nxt[s], by_member(r["aux"], s)) for s in subs]
        else:
            first = [by_member(r["prev"], s) for s in subs]
            second = cur
        feats = [jnp.concatenate([((first[s] - mean) / std).astype(BF16), ((second[s] - mean) / std).astype(BF16)], axis=1) for s in subs]
        hid = [silu(mm(f, r["w_grid"][...])) for f in feats]
        v = [norm(mm(h, r["w_grid_out"][...])).astype(BF16) for h in hid]
        pre = []
        for s in subs:
            recv = mm(r["mesh"][rows_of(s, CELLS), :], r["wf"][2 * LAT:, :])
            both = mm(r["g2m"][rows_of(s, ROWS), :], r["wf"][:LAT, :]) + mm(v[s], r["wf"][LAT:2 * LAT, :])
            pre.append(both + tile4(recv))
        self_hid = [silu(mm(x, r["w_self"][0])) for x in v]
        hid = [silu(p) for p in pre]
        upd = [mm(h, r["wf_out"][...]) for h in hid]
        self_upd = [mm(h, r["w_self"][1]) for h in self_hid]
        total = []
        for s in subs:
            edge = add_to(r["g2m"][rows_of(s, ROWS), :], norm(upd[s])).astype(F32)
            parts = [edge[k * CELLS:(k + 1) * CELLS] for k in range(RATIO)]
            total.append((parts[0] + parts[1] + parts[2] + parts[3]).astype(BF16))
        mesh = [r["mesh"][rows_of(s, CELLS), :] for s in subs]
        pre = [mm(mesh[s], r["wf_node"][:LAT, :]) + mm(total[s], r["wf_node"][LAT:, :]) for s in subs]
        for s in subs:
            r["grid_new"][rows_of(s, ROWS), :] = add_to(v[s], norm(self_upd[s]))
        hid = [silu(p) for p in pre]
        upd = [mm(h, r["wf_node_out"][...]) for h in hid]
        for s in subs:
            r["h_out"][s, 0] = add_to(mesh[s], norm(upd[s]))


def grid_call(arrays, weights, decode, encode, name):
    tiles = arrays["cur"].shape[0] // ROWS
    lead = tiles // 2
    step_rows = SUB * ROWS
    node_spec = pl.BlockSpec((SUB, 1, CELLS, LAT), lambda i: (i % (lead // SUB), i // (lead // SUB), 0, 0))
    special = {
        "h_in": node_spec,
        "mesh": pl.BlockSpec((SUB * CELLS, LAT), lambda i: (i, 0)),
        "g2m": pl.BlockSpec((step_rows, LAT), lambda i: (i + 1, 0)),
        "m2g": pl.BlockSpec((step_rows, LAT), lambda i: (i + 1 + tiles // SUB, 0)),
    }
    names, specs, operands = [], [], []
    for key, arr in arrays.items():
        names.append(key)
        operands.append(arr)
        specs.append(special.get(key) or pl.BlockSpec((step_rows, arr.shape[1]), lambda i: (i, 0)))
    for key, arr in weights.items():
        names.append(key)
        operands.append(arr)
        specs.append(pl.BlockSpec(arr.shape, functools.partial(lambda nd, i: (0,) * nd, arr.ndim)))
    out_specs, out_shapes = [], []
    if decode:
        names.append("next")
        out_specs.append(pl.BlockSpec((step_rows, VARS), lambda i: (i, 0)))
        out_shapes.append(jax.ShapeDtypeStruct((tiles * ROWS, VARS), F32))
    if encode:
        names += ["grid_new", "h_out"]
        out_specs += [pl.BlockSpec((step_rows, LAT), lambda i: (i, 0)), node_spec]
        out_shapes += [jax.ShapeDtypeStruct((tiles * ROWS, LAT), BF16), jax.ShapeDtypeStruct((lead, 2, CELLS, LAT), BF16)]
    return pl.pallas_call(
        functools.partial(grid_kernel, tuple(names), decode, encode),
        grid=(tiles // SUB,),
        in_specs=specs,
        out_specs=out_specs,
        out_shape=out_shapes,
        compiler_params=pltpu.CompilerParams(vmem_limit_bytes=VMEM_LIMIT),
        name=name,
    )(*operands)


def proc_kernel(first_edge, h_in, lat, w_ei, w_eo, w_ni, w_no, h_out, edge, mesh, proj, recv, total, turn, halo, b_ei, b_eo, b_ni, b_no, w_sem, e_sem, s_sem, r_sem):
    ring = 4
    me = lax.axis_index("gp")
    right = lax.rem(me + 1, ring)
    left = lax.rem(me + ring - 1, ring)

    def weight_copies(layer, slot):
        pairs = ((w_ei, b_ei), (w_eo, b_eo), (w_ni, b_ni), (w_no, b_no))
        return [pltpu.make_async_copy(src.at[layer], dst.at[slot], w_sem.at[slot, i]) for i, (src, dst) in enumerate(pairs)]

    edge_copies = [pltpu.make_async_copy(lat.at[pl.ds(first_edge + k * NODES, NODES)], edge.at[k], e_sem.at[k]) for k in range(OFFS)]
    for copy in weight_copies(1, 1) + edge_copies:
        copy.start()

    barrier = pltpu.get_barrier_semaphore()
    for peer in (left, right):
        pl.semaphore_signal(barrier, inc=1, device_id={"gp": peer}, device_id_type=pl.DeviceIdType.MESH)

    cols = [slice(c * LANES, (c + 1) * LANES) for c in range(LAT // LANES)]
    for c, col in enumerate(cols):
        for q in range(Q):
            turn[c, pl.ds(q, RLOC, stride=Q), :] = h_in[q, :, col].astype(F32)
    for c, col in enumerate(cols):
        mesh[:, col] = turn[c].astype(BF16)
    pl.semaphore_wait(barrier, 2)
    for copy in weight_copies(1, 1):
        copy.wait()

    def project(slot):
        for c in range(2):
            rows = pl.ds(c * 512, 512)
            nodes = mesh[rows, :]
            proj[pl.ds(8 + c * 512, 512), :] = mm(nodes, b_ei[slot, LAT:2 * LAT, :])
            recv[rows, :] = mm(nodes, b_ei[slot, 2 * LAT:, :])

    project(1)
    for copy in edge_copies:
        copy.wait()

    def edge_tile(slot, t):
        start = pl.multiple_of(t * TILE, TILE)
        rows = pl.ds(start, TILE)
        at_recv = recv[rows, :]
        here = proj[pl.ds(start + 8, TILE), :].reshape(TILE // Q, Q, LAT)

        def sender(k):
            if k == 0:
                return proj[pl.ds(start + 16, TILE), :]
            if k == 1:
                return proj[rows, :]
            shift = {2: Q - 1, 3: 1, 4: Q - 2, 5: 2}[k]
            return pltpu.roll(here, shift, 1).reshape(TILE, LAT)

        w_first = b_ei[slot, :LAT, :]
        w_second = b_eo[slot]
        old, pre = [], []
        for c in range(3):
            pair = edge[2 * c:2 * c + 2, rows, :].reshape(2 * TILE, LAT)
            old.append(pair)
            terms = jnp.concatenate([sender(2 * c) + at_recv, sender(2 * c + 1) + at_recv], axis=0)
            pre.append(mm(pair, w_first) + terms)
        upd = [mm(silu(p), w_second) for p in pre]
        acc = None
        for c in range(3):
            new = add_to(old[c], norm(upd[c]))
            edge[2 * c:2 * c + 2, rows, :] = new.reshape(2, TILE, LAT)
            wide = new.astype(F32)
            part = wide[:TILE] + wide[TILE:]
            acc = part if acc is None else acc + part
        total[rows, :] = acc.astype(BF16)

    def update_nodes(slot, last):
        chunks = [pl.ds(c * 512, 512) for c in range(2)]
        nodes = [mesh[rows, :] for rows in chunks]
        pre = [mm(nodes[c], b_ni[slot, :LAT, :]) + mm(total[chunks[c], :], b_ni[slot, LAT:, :]) for c in range(2)]
        upd = [mm(silu(p), b_no[slot]) for p in pre]
        for c in range(2):
            new = add_to(nodes[c], norm(upd[c]))
            if last:
                for d, col in enumerate(cols):
                    turn[d, chunks[c], :] = new[:, col].astype(F32)
            else:
                mesh[chunks[c], :] = new
                proj[pl.ds(8 + c * 512, 512), :] = mm(new, b_ei[1 - slot, LAT:2 * LAT, :])
                recv[chunks[c], :] = mm(new, b_ei[1 - slot, 2 * LAT:, :])

    def layer(l, last):
        slot = lax.rem(l, 2)
        if not last:
            for copy in weight_copies(l + 1, 1 - slot):
                copy.start()
        sends = [
            pltpu.make_async_remote_copy(
                src_ref=proj.at[pl.ds(first, 8)],
                dst_ref=halo.at[slot, side],
                send_sem=s_sem.at[side],
                recv_sem=r_sem.at[slot, side],
                device_id={"gp": peer},
                device_id_type=pl.DeviceIdType.MESH)
            for side, first, peer in ((0, NODES, right), (1, 8, left))]
        for send in sends:
            send.start()

        def pair(base):
            def body(i, carry):
                edge_tile(slot, lax.rem(i + base, NODES // TILE))
                return carry
            lax.fori_loop(0, 2, body, 0)

        pair(1)
        for send in sends:
            send.wait_recv()
        below = halo[slot, 0]
        above = halo[slot, 1]
        proj[0:8, :] = jnp.where(me == 0, pltpu.roll(below, 1, 0), below)
        proj[8 + NODES:16 + NODES, :] = jnp.where(me == ring - 1, pltpu.roll(above, Q - 1, 0), above)
        pair(3)
        for send in sends:
            send.wait_send()
        if not last:
            for copy in weight_copies(l + 1, 1 - slot):
                copy.wait()
        update_nodes(slot, last)

    def loop_body(l, carry):
        layer(l, False)
        return carry

    lax.fori_loop(1, LAYERS, loop_body, 0)
    layer(jnp.int32(LAYERS), True)
    for c, col in enumerate(cols):
        for q in range(Q):
            h_out[q, :, col] = turn[c, pl.ds(q, RLOC, stride=Q), :].astype(BF16)


def processor(h_in, lat, first_edge, w_edge_in, w_edge_out, w_node_in, w_node_out):
    hbm = pl.BlockSpec(memory_space=pl.ANY)
    vmem = pl.BlockSpec(memory_space=pltpu.VMEM)
    rows = NODES * (OFFS * 2 + 8)
    return pl.pallas_call(
        functools.partial(proc_kernel, first_edge),
        in_specs=[vmem, hbm, hbm, hbm, hbm, hbm],
        out_specs=vmem,
        out_shape=jax.ShapeDtypeStruct((Q, RLOC, LAT), BF16),
        scratch_shapes=[
            pltpu.VMEM((OFFS, NODES, LAT), BF16),
            pltpu.VMEM((NODES, LAT), BF16),
            pltpu.VMEM((NODES + 16, LAT), F32),
            pltpu.VMEM((NODES, LAT), F32),
            pltpu.VMEM((NODES, LAT), BF16),
            pltpu.VMEM((LAT // LANES, NODES, LANES), F32),
            pltpu.VMEM((2, 2, 8, LAT), F32),
            pltpu.VMEM((2, 3 * LAT, LAT), BF16),
            pltpu.VMEM((2, LAT, LAT), BF16),
            pltpu.VMEM((2, 2 * LAT, LAT), BF16),
            pltpu.VMEM((2, LAT, LAT), BF16),
            pltpu.SemaphoreType.DMA((2, 4)),
            pltpu.SemaphoreType.DMA((OFFS,)),
            pltpu.SemaphoreType.DMA((2,)),
            pltpu.SemaphoreType.DMA((2, 2)),
        ],
        compiler_params=pltpu.CompilerParams(collective_id=0, has_side_effects=True, vmem_limit_bytes=VMEM_LIMIT),
        cost_estimate=pl.CostEstimate(flops=2 * LAYERS * rows * LAT * LAT, bytes_accessed=60 * 2 ** 20, transcendentals=0),
        name="processor",
    )(h_in, lat, w_edge_in, w_edge_out, w_node_in, w_node_out)


def solution(mesh):
    ring = mesh.shape["gp"]
    row_spec = P(("dp", "gp"))
    edge_spec = P(("dp", "gp"), None, None)
    whole = P()

    def exchange(x):
        return lax.all_to_all(x, "gp", 0, 0)

    def member_order(x):
        return x.reshape(-1, CELLS, RATIO, x.shape[-1]).swapaxes(1, 2).reshape(-1, x.shape[-1])

    def wide(x):
        return jnp.pad(x, ((0, 0), (0, LANES - x.shape[1])))

    def local_run(x_prev, x_cur, forcing, grid_static, g2m_feat, m2g_feat, mesh_feat, mesh_edge_feat, norm_stats, w_grid_in, w_mesh_in, w_eemb_in, w_embed_out, w_edge_in, w_edge_out, w_node_in, w_node_out, w_grid_self, w_out_hidden, w_out_final):
        grid_dev = x_prev.shape[0]
        mesh_dev = mesh_feat.shape[0]
        half = mesh_dev // 2
        packed = jnp.concatenate([mesh_feat, g2m_feat.reshape(mesh_dev, RATIO * 4)], axis=1).astype(BF16)
        head = lax.ppermute(packed[:half], "gp", [(s, (s - 1) % ring) for s in range(ring)])
        packed = jnp.concatenate([packed[half:], head], axis=0)
        node_rows = packed[:, :3]
        g2m_rows = member_order(packed[:, 3:].reshape(grid_dev, 4))
        m2g_rows = member_order(m2g_feat.astype(BF16))
        edges = mesh_edge_feat.astype(BF16).reshape(2, ring, RLOC, OFFS * 4).swapaxes(0, 1)
        edges = exchange(edges).reshape(Q, RLOC, OFFS, 4)
        edges = jnp.roll(edges, -1, axis=0)
        edge_rows = edges.transpose(2, 1, 0, 3).reshape(OFFS * NODES, 4)
        feats = jnp.concatenate([wide(node_rows), wide(g2m_rows), wide(m2g_rows), wide(edge_rows)], axis=0)
        pad_in = jnp.stack([jnp.pad(w, ((0, LANES - w.shape[0]), (0, 0))) for w in (w_mesh_in, w_eemb_in[0], w_eemb_in[1], w_eemb_in[2])])
        starts = (mesh_dev, mesh_dev + grid_dev, mesh_dev + 2 * grid_dev)
        lat = embed_static(feats, pad_in, w_embed_out[1:], starts)

        stats = jnp.pad(norm_stats, ((0, 0), (0, LANES - VARS)), constant_values=0.0)
        stats = stats.at[1, VARS:].set(1.0)
        w_grid = jnp.concatenate([
            w_grid_in[:VARS], jnp.zeros((LANES - VARS, LAT), BF16), w_grid_in[VARS:],
            jnp.zeros((2 * LANES - VARS - (LANES - VARS) - (w_grid_in.shape[0] - VARS), LAT), BF16)], axis=0)
        w_final = jnp.pad(w_out_final, ((0, 0), (0, LANES - VARS)))
        last = w_edge_in.shape[0] - 1
        enc_w = {"stats": stats, "w_grid": w_grid, "w_grid_out": w_embed_out[0], "wf": w_edge_in[0], "wf_out": w_edge_out[0], "wf_node": w_node_in[0], "wf_node_out": w_node_out[0], "w_self": w_grid_self}
        dec_w = {"stats": stats, "wl": w_edge_in[last], "wl_out": w_edge_out[last], "wl_node": w_node_in[last], "wl_node_out": w_node_out[last], "w_hidden": w_out_hidden, "w_final": w_final}
        prev = wide(x_prev)
        cur = wide(jnp.concatenate([x_cur, forcing[:, 0, :], grid_static], axis=1))
        aux = wide(jnp.concatenate([jnp.zeros((grid_dev, VARS), F32), forcing[:, 1, :], grid_static], axis=1))

        def process(h):
            h = exchange(h).reshape(Q, RLOC, LAT)
            h = processor(h, lat, starts[2], w_edge_in, w_edge_out, w_node_in, w_node_out)
            return exchange(h.reshape(ring, 2, RLOC, LAT))

        grid_lat, h = grid_call({"cur": cur, "prev": prev, "g2m": lat, "mesh": lat}, enc_w, False, True, "encode")
        h = process(h)
        x_next, grid_lat, h = grid_call({"cur": cur, "h_in": h, "grid_cur": grid_lat, "m2g": lat, "aux": aux, "g2m": lat, "mesh": lat}, {**dec_w, **enc_w}, True, True, "decode_encode")
        h = process(h)
        x_after, = grid_call({"cur": wide(x_next), "h_in": h, "grid_cur": grid_lat, "m2g": lat}, dec_w, True, False, "decode")
        return x_next, x_after

    in_specs = (row_spec, row_spec, edge_spec, row_spec, row_spec, row_spec, row_spec, edge_spec, whole) + (whole,) * 11
    return jax.shard_map(local_run, mesh=mesh, in_specs=in_specs, out_specs=(row_spec, row_spec), check_vma=False)
```

```python
import functools

import jax
import jax.numpy as jnp
from jax import lax
from jax.experimental import pallas as pl
from jax.experimental.pallas import tpu as pltpu
from jax.sharding import PartitionSpec as P

F32 = jnp.float32
BF16 = jnp.bfloat16
LAT = 512
VARS = 83
LANES = 128
CELLS = 128
RATIO = 4
ROWS = CELLS * RATIO
SUB = 2
Q = 8
RLOC = 128
NODES = Q * RLOC
OFFS = 6
LAYERS = 12
TILE = 256
CHUNK = 512
LAG_B = 1
LAG_C = 2
VMEM_LIMIT = 60 * 1024 * 1024


def mm(lhs, rhs):
    return jnp.dot(lhs, rhs, preferred_element_type=F32)


def silu_twice(x):
    return (x + x * jnp.tanh(x)).astype(BF16)


def half_norm(y):
    centred = y - jnp.sum(y, axis=-1, keepdims=True) * (1.0 / LAT)
    spread = jnp.sum(centred * centred, axis=-1, keepdims=True)
    return centred * (lax.rsqrt(spread + LAT * 1e-5) * (0.5 * LAT ** 0.5))


def add_to(base, update):
    return (base.astype(F32) + update).astype(BF16)


def mm_features(feats, weight):
    return lax.dot_general(feats, weight, (((0,), (0,)), ((), ())), preferred_element_type=F32)


def embed_kernel(x_ref, w_in_ref, w_out_ref, o_ref):
    halves = [slice(s * ROWS, (s + 1) * ROWS) for s in range(SUB)]
    hid = [silu_twice(mm_features(0.5 * x_ref[:, cols], w_in_ref[0])) for cols in halves]
    upd = [mm(h, w_out_ref[0]) for h in hid]
    for s in range(SUB):
        o_ref[halves[s], :] = half_norm(upd[s]).astype(BF16)


def embed_static(feats, w_in, w_out, starts, name):
    depth, rows = feats.shape
    block = SUB * ROWS

    def kind(i):
        return sum((i >= s // block).astype(jnp.int32) for s in starts) if starts else 0

    return pl.pallas_call(
        embed_kernel,
        grid=(rows // block,),
        in_specs=[
            pl.BlockSpec((depth, block), lambda i: (0, i)),
            pl.BlockSpec((1, depth, LAT), lambda i: (kind(i), 0, 0)),
            pl.BlockSpec((1, LAT, LAT), lambda i: (kind(i), 0, 0)),
        ],
        out_specs=pl.BlockSpec((block, LAT), lambda i: (i, 0)),
        out_shape=jax.ShapeDtypeStruct((rows, LAT), BF16),
        compiler_params=pltpu.CompilerParams(vmem_limit_bytes=VMEM_LIMIT),
        cost_estimate=pl.CostEstimate(flops=6 * rows * LAT * LAT, bytes_accessed=2 * rows * LAT, transcendentals=0),
        name=name,
    )(feats, w_in, w_out)


def rows_of(sub, size):
    return pl.ds(sub * size, size)


LANE_COLS = [slice(c * LANES, (c + 1) * LANES) for c in range(LAT // LANES)]


def spread(buf, sub, cell_rows):
    for c, col in enumerate(LANE_COLS):
        for k in range(RATIO):
            buf[c, pl.ds(sub * ROWS + k, CELLS, stride=RATIO), :] = cell_rows[:, col]
    return jnp.concatenate([buf[c, rows_of(sub, ROWS), :] for c in range(len(LANE_COLS))], axis=1)


def gather_sum(buf, sub, node_rows):
    for c, col in enumerate(LANE_COLS):
        buf[c, rows_of(sub, ROWS), :] = node_rows[:, col]
    sums = []
    for c in range(len(LANE_COLS)):
        parts = [buf[c, pl.ds(sub * ROWS + k, CELLS, stride=RATIO), :] for k in range(RATIO)]
        sums.append(parts[0] + parts[1] + parts[2] + parts[3])
    return jnp.concatenate(sums, axis=1).astype(BF16)


FEAT_CUR = 88
FEAT_FORCE = 176
FEAT_ROWS = 192


def grid_kernel(names, decode, encode, *refs):
    r = dict(zip(names, refs))
    mean, std, diff_mean, diff_std = (r["stats"][:, i:i + 1] for i in range(4))
    subs = range(SUB)
    cols = [slice(s * ROWS, (s + 1) * ROWS) for s in subs]
    cur = [r["cur"][:, c] for c in cols]
    if decode:
        grid_cur = [r["grid_cur"][rows_of(s, ROWS), :] for s in subs]
        pre = []
        for s in subs:
            send = mm(r["h_in"][s, 0], r["wl"][LAT:2 * LAT, :])
            both = mm(r["m2g"][rows_of(s, ROWS), :], r["wl"][:LAT, :]) + mm(grid_cur[s], r["wl"][2 * LAT:, :])
            pre.append(both + spread(r["buf_send"], s, send))
        hid = [silu_twice(p) for p in pre]
        upd = [mm(h, r["wl_out"][...]) for h in hid]
        edge = [add_to(r["m2g"][rows_of(s, ROWS), :], half_norm(upd[s])) for s in subs]
        pre = [mm(grid_cur[s], r["wl_node"][:LAT, :]) + mm(edge[s], r["wl_node"][LAT:, :]) for s in subs]
        hid = [silu_twice(p) for p in pre]
        upd = [mm(h, r["wl_node_out"][...]) for h in hid]
        out = [add_to(grid_cur[s], half_norm(upd[s])) for s in subs]
        hid = [silu_twice(mm(o, r["w_hidden"][...])) for o in out]
        pred = [mm(h, r["w_final"][...]).T[:VARS] for h in hid]
        nxt = [cur[s] + diff_std * pred[s] + diff_mean for s in subs]
        for s in subs:
            r["next"][:, cols[s]] = nxt[s]
    if encode:
        if decode:
            first, second = cur, nxt
        else:
            first, second = [r["prev"][:, c] for c in cols], cur
        table = r["buf_feat"]
        feats = []
        for s in subs:
            table[VARS - 3:FEAT_CUR, cols[s]] = jnp.zeros((8, ROWS), F32)
            table[FEAT_FORCE - 8:FEAT_FORCE, cols[s]] = jnp.zeros((8, ROWS), F32)
            table[:VARS, cols[s]] = (first[s] - mean) / std
            table[FEAT_CUR:FEAT_CUR + VARS, cols[s]] = (second[s] - mean) / std
            table[FEAT_FORCE:, cols[s]] = r["force"][:, cols[s]]
            feats.append(0.5 * table[:, cols[s]].astype(BF16))
        hid = [silu_twice(mm_features(f, r["w_grid"][...])) for f in feats]
        v = [half_norm(mm(h, r["w_grid_out"][...])).astype(BF16) for h in hid]
        pre = []
        for s in subs:
            recv = mm(r["mesh"][rows_of(s, CELLS), :], r["wf"][2 * LAT:, :])
            both = mm(r["g2m"][rows_of(s, ROWS), :], r["wf"][:LAT, :]) + mm(v[s], r["wf"][LAT:2 * LAT, :])
            pre.append(both + spread(r["buf_recv"], s, recv))
        self_hid = [silu_twice(mm(x, r["w_self"][0])) for x in v]
        hid = [silu_twice(p) for p in pre]
        upd = [mm(h, r["wf_out"][...]) for h in hid]
        self_upd = [mm(h, r["w_self"][1]) for h in self_hid]
        total = [gather_sum(r["buf_sum"], s, add_to(r["g2m"][rows_of(s, ROWS), :], half_norm(upd[s])).astype(F32)) for s in subs]
        mesh = [r["mesh"][rows_of(s, CELLS), :] for s in subs]
        pre = [mm(mesh[s], r["wf_node"][:LAT, :]) + mm(total[s], r["wf_node"][LAT:, :]) for s in subs]
        for s in subs:
            r["grid_new"][rows_of(s, ROWS), :] = add_to(v[s], half_norm(self_upd[s]))
        hid = [silu_twice(p) for p in pre]
        upd = [mm(h, r["wf_node_out"][...]) for h in hid]
        for s in subs:
            r["h_out"][s, 0] = add_to(mesh[s], half_norm(upd[s]))


def grid_call(arrays, weights, decode, encode, name):
    tiles = arrays["cur"].shape[1] // ROWS
    lead = tiles // 2
    step_rows = SUB * ROWS
    node_spec = pl.BlockSpec((SUB, 1, CELLS, LAT), lambda i: (i % (lead // SUB), i // (lead // SUB), 0, 0))
    special = {
        "h_in": node_spec,
        "grid_cur": pl.BlockSpec((step_rows, LAT), lambda i: (i, 0)),
        "mesh": pl.BlockSpec((SUB * CELLS, LAT), lambda i: (i, 0)),
        "g2m": pl.BlockSpec((step_rows, LAT), lambda i: (i + 1, 0)),
        "m2g": pl.BlockSpec((step_rows, LAT), lambda i: (i + 1 + tiles // SUB, 0)),
    }
    names, specs, operands = [], [], []
    for key, arr in arrays.items():
        names.append(key)
        operands.append(arr)
        specs.append(special.get(key) or pl.BlockSpec((arr.shape[0], step_rows), lambda i: (0, i)))
    for key, arr in weights.items():
        names.append(key)
        operands.append(arr)
        specs.append(pl.BlockSpec(arr.shape, functools.partial(lambda nd, i: (0,) * nd, arr.ndim)))
    out_specs, out_shapes, scratch = [], [], []
    wide = pltpu.VMEM((len(LANE_COLS), step_rows, LANES), F32)
    if decode:
        names.append("next")
        out_specs.append(pl.BlockSpec((VARS, step_rows), lambda i: (0, i)))
        out_shapes.append(jax.ShapeDtypeStruct((VARS, tiles * ROWS), F32))
    if encode:
        names += ["grid_new", "h_out"]
        out_specs += [pl.BlockSpec((step_rows, LAT), lambda i: (i, 0)), node_spec]
        out_shapes += [jax.ShapeDtypeStruct((tiles * ROWS, LAT), BF16), jax.ShapeDtypeStruct((lead, 2, CELLS, LAT), BF16)]
    if decode:
        names.append("buf_send")
        scratch.append(wide)
    if encode:
        names += ["buf_recv", "buf_sum", "buf_feat"]
        scratch += [wide, wide, pltpu.VMEM((FEAT_ROWS, step_rows), F32)]
    return pl.pallas_call(
        functools.partial(grid_kernel, tuple(names), decode, encode),
        grid=(tiles // SUB,),
        in_specs=specs,
        out_specs=out_specs,
        out_shape=out_shapes,
        scratch_shapes=scratch,
        compiler_params=pltpu.CompilerParams(vmem_limit_bytes=VMEM_LIMIT),
        cost_estimate=pl.CostEstimate(flops=2 * 7 * tiles * ROWS * LAT * LAT * (decode + encode), bytes_accessed=2 ** 24, transcendentals=0),
        name=name,
    )(*operands)


def proc_kernel(first_edge, h_in, lat, w_ei, w_eo, w_ni, w_no, h_out, edge, mesh, proj, recv, total, turn, halo, b_ei, b_eo, b_ni, b_no, w_sem, e_sem, s_sem, r_sem):
    ring = 4
    me = lax.axis_index("gp")
    right = lax.rem(me + 1, ring)
    left = lax.rem(me + ring - 1, ring)

    def weight_copies(layer, slot):
        pairs = ((w_ei, b_ei), (w_eo, b_eo), (w_ni, b_ni), (w_no, b_no))
        return [pltpu.make_async_copy(src.at[layer], dst.at[slot], w_sem.at[slot, i]) for i, (src, dst) in enumerate(pairs)]

    edge_copies = [pltpu.make_async_copy(lat.at[pl.ds(first_edge + k * NODES, NODES)], edge.at[k], e_sem.at[k]) for k in range(OFFS)]
    for copy in weight_copies(1, 1) + edge_copies:
        copy.start()

    barrier = pltpu.get_barrier_semaphore()
    for peer in (left, right):
        pl.semaphore_signal(barrier, inc=1, device_id={"gp": peer}, device_id_type=pl.DeviceIdType.MESH)

    for c, col in enumerate(LANE_COLS):
        for q in range(Q):
            turn[c, pl.ds(q, RLOC, stride=Q), :] = h_in[q, :, col].astype(F32)
    for c, col in enumerate(LANE_COLS):
        mesh[:, col] = turn[c].astype(BF16)
    pl.semaphore_wait(barrier, 2)
    for copy in weight_copies(1, 1):
        copy.wait()

    def project(slot):
        for c in range(2):
            rows = pl.ds(c * 512, 512)
            nodes = mesh[rows, :]
            proj[pl.ds(8 + c * 512, 512), :] = mm(nodes, b_ei[slot, LAT:2 * LAT, :])
            recv[rows, :] = mm(nodes, b_ei[slot, 2 * LAT:, :])

    project(1)
    for copy in edge_copies:
        copy.wait()

    def edge_tile(slot, t):
        start = pl.multiple_of(t * TILE, TILE)
        rows = pl.ds(start, TILE)
        at_recv = recv[rows, :]
        here = proj[pl.ds(start + 8, TILE), :].reshape(TILE // Q, Q, LAT)

        def sender(k):
            if k == 0:
                return proj[pl.ds(start + 16, TILE), :]
            if k == 1:
                return proj[rows, :]
            shift = {2: Q - 1, 3: 1, 4: Q - 2, 5: 2}[k]
            return pltpu.roll(here, shift, 1).reshape(TILE, LAT)

        w_first = b_ei[slot, :LAT, :]
        w_second = b_eo[slot]
        chunks = OFFS * TILE // CHUNK
        per = CHUNK // TILE
        old, hid, upd = {}, {}, {}
        acc = [None]

        def stage_a(c):
            pair = edge[per * c:per * c + per, rows, :].reshape(CHUNK, LAT)
            old[c] = pair
            terms = jnp.concatenate([sender(per * c + j) + at_recv for j in range(per)], axis=0)
            hid[c] = silu_twice(mm(pair, w_first) + terms)

        def stage_b(c):
            upd[c] = mm(hid[c], w_second)

        def stage_c(c):
            new = add_to(old[c], half_norm(upd[c]))
            edge[per * c:per * c + per, rows, :] = new.reshape(per, TILE, LAT)
            wide = new.astype(F32)
            for j in range(per):
                part = wide[j * TILE:(j + 1) * TILE]
                acc[0] = part if acc[0] is None else acc[0] + part

        for c in range(chunks + LAG_C):
            if c < chunks:
                stage_a(c)
            if LAG_B <= c < chunks + LAG_B:
                stage_b(c - LAG_B)
            if LAG_C <= c:
                stage_c(c - LAG_C)
        total[rows, :] = acc[0].astype(BF16)

    def update_nodes(slot, last):
        chunks = [pl.ds(c * 512, 512) for c in range(2)]
        nodes = [mesh[rows, :] for rows in chunks]
        hid = [silu_twice(mm(nodes[c], b_ni[slot, :LAT, :]) + mm(total[chunks[c], :], b_ni[slot, LAT:, :])) for c in range(2)]
        upd = [mm(h, b_no[slot]) for h in hid]
        for c in range(2):
            new = add_to(nodes[c], half_norm(upd[c]))
            if last:
                for d, col in enumerate(LANE_COLS):
                    turn[d, chunks[c], :] = new[:, col].astype(F32)
            else:
                mesh[chunks[c], :] = new
                proj[pl.ds(8 + c * 512, 512), :] = mm(new, b_ei[1 - slot, LAT:2 * LAT, :])
                recv[chunks[c], :] = mm(new, b_ei[1 - slot, 2 * LAT:, :])

    def layer(l, last):
        slot = lax.rem(l, 2)
        if not last:
            for copy in weight_copies(l + 1, 1 - slot):
                copy.start()
        sends = [
            pltpu.make_async_remote_copy(
                src_ref=proj.at[pl.ds(first, 8)],
                dst_ref=halo.at[slot, side],
                send_sem=s_sem.at[side],
                recv_sem=r_sem.at[slot, side],
                device_id={"gp": peer},
                device_id_type=pl.DeviceIdType.MESH)
            for side, first, peer in ((0, NODES, right), (1, 8, left))]
        for send in sends:
            send.start()

        def pair(base):
            def body(i, carry):
                edge_tile(slot, lax.rem(i + base, NODES // TILE))
                return carry
            lax.fori_loop(0, 2, body, 0)

        pair(1)
        for send in sends:
            send.wait_recv()
        below = halo[slot, 0]
        above = halo[slot, 1]
        proj[0:8, :] = jnp.where(me == 0, pltpu.roll(below, 1, 0), below)
        proj[8 + NODES:16 + NODES, :] = jnp.where(me == ring - 1, pltpu.roll(above, Q - 1, 0), above)
        pair(3)
        for send in sends:
            send.wait_send()
        if not last:
            for copy in weight_copies(l + 1, 1 - slot):
                copy.wait()
        update_nodes(slot, last)

    def loop_body(l, carry):
        layer(l, False)
        return carry

    lax.fori_loop(1, LAYERS, loop_body, 0)
    layer(jnp.int32(LAYERS), True)
    for c, col in enumerate(LANE_COLS):
        for q in range(Q):
            h_out[q, :, col] = turn[c, pl.ds(q, RLOC, stride=Q), :].astype(BF16)


def processor(h_in, lat, first_edge, w_edge_in, w_edge_out, w_node_in, w_node_out):
    hbm = pl.BlockSpec(memory_space=pl.ANY)
    vmem = pl.BlockSpec(memory_space=pltpu.VMEM)
    rows = NODES * (OFFS * 2 + 8)
    return pl.pallas_call(
        functools.partial(proc_kernel, first_edge),
        in_specs=[vmem, hbm, hbm, hbm, hbm, hbm],
        out_specs=vmem,
        out_shape=jax.ShapeDtypeStruct((Q, RLOC, LAT), BF16),
        scratch_shapes=[
            pltpu.VMEM((OFFS, NODES, LAT), BF16),
            pltpu.VMEM((NODES, LAT), BF16),
            pltpu.VMEM((NODES + 16, LAT), F32),
            pltpu.VMEM((NODES, LAT), F32),
            pltpu.VMEM((NODES, LAT), BF16),
            pltpu.VMEM((LAT // LANES, NODES, LANES), F32),
            pltpu.VMEM((2, 2, 8, LAT), F32),
            pltpu.VMEM((2, 3 * LAT, LAT), BF16),
            pltpu.VMEM((2, LAT, LAT), BF16),
            pltpu.VMEM((2, 2 * LAT, LAT), BF16),
            pltpu.VMEM((2, LAT, LAT), BF16),
            pltpu.SemaphoreType.DMA((2, 4)),
            pltpu.SemaphoreType.DMA((OFFS,)),
            pltpu.SemaphoreType.DMA((2,)),
            pltpu.SemaphoreType.DMA((2, 2)),
        ],
        compiler_params=pltpu.CompilerParams(collective_id=0, has_side_effects=True, vmem_limit_bytes=VMEM_LIMIT),
        cost_estimate=pl.CostEstimate(flops=2 * LAYERS * rows * LAT * LAT, bytes_accessed=60 * 2 ** 20, transcendentals=0),
        name="processor",
    )(h_in, lat, w_edge_in, w_edge_out, w_node_in, w_node_out)


def solution(mesh):
    ring = mesh.shape["gp"]
    row_spec = P(("dp", "gp"))
    edge_spec = P(("dp", "gp"), None, None)
    whole = P()

    def exchange(x):
        return lax.all_to_all(x, "gp", 0, 0)

    def local_run(x_prev, x_cur, forcing, grid_static, g2m_feat, m2g_feat, mesh_feat, mesh_edge_feat, norm_stats, w_grid_in, w_mesh_in, w_eemb_in, w_embed_out, w_edge_in, w_edge_out, w_node_in, w_node_out, w_grid_self, w_out_hidden, w_out_final):
        grid_dev = x_prev.shape[0]
        mesh_dev = mesh_feat.shape[0]
        half = mesh_dev // 2
        deep = 8

        def padded(x):
            return jnp.pad(x, ((0, deep - x.shape[0]), (0, 0)))

        edges = mesh_edge_feat.astype(BF16).transpose(1, 2, 0).reshape(OFFS * 4, 2, ring, RLOC).transpose(2, 0, 1, 3)
        edges = exchange(edges)
        edges = edges.reshape(ring, OFFS, 4, 2, RLOC).transpose(2, 1, 4, 0, 3).reshape(4, OFFS * RLOC, Q)
        edges = padded(jnp.roll(edges, -1, axis=2).reshape(4, OFFS * NODES))
        node_rows = mesh_feat.astype(BF16).T
        g2m_rows = g2m_feat.astype(BF16).T
        head = jnp.concatenate([node_rows[:, :half]] + [g2m_rows[:, k * half:(k + 1) * half] for k in range(RATIO)], axis=0)
        head = lax.ppermute(head, "gp", [(s, (s - 1) % ring) for s in range(ring)])
        node_rows = padded(jnp.concatenate([node_rows[:, half:], head[:3]], axis=1))
        g2m_rows = padded(jnp.concatenate([g2m_rows[:, RATIO * half:]] + [head[3 + 4 * k:7 + 4 * k] for k in range(RATIO)], axis=1))
        feats = jnp.concatenate([node_rows, g2m_rows, padded(m2g_feat.astype(BF16).T)], axis=1)
        lat = embed_static(feats, jnp.stack([padded(w_mesh_in), padded(w_eemb_in[0]), padded(w_eemb_in[1])]), w_embed_out[1:4], (mesh_dev, mesh_dev + grid_dev), "embed")
        edge_lat = embed_static(edges, padded(w_eemb_in[2])[None], w_embed_out[4:5], (), "embed_edges")

        w_grid = jnp.concatenate([
            jnp.pad(w_grid_in[:VARS], ((0, FEAT_CUR - VARS), (0, 0))),
            jnp.pad(w_grid_in[VARS:2 * VARS], ((0, FEAT_CUR - VARS), (0, 0))),
            padded(w_grid_in[2 * VARS:2 * VARS + 5]), padded(w_grid_in[2 * VARS + 5:])], axis=0)
        w_final = jnp.pad(w_out_final, ((0, 0), (0, LANES - VARS)))
        last = w_edge_in.shape[0] - 1
        stats = norm_stats.T
        enc_w = {"stats": stats, "w_grid": w_grid, "w_grid_out": w_embed_out[0], "wf": w_edge_in[0], "wf_out": w_edge_out[0], "wf_node": w_node_in[0], "wf_node_out": w_node_out[0], "w_self": w_grid_self}
        dec_w = {"stats": stats, "wl": w_edge_in[last], "wl_out": w_edge_out[last], "wl_node": w_node_in[last], "wl_node_out": w_node_out[last], "w_hidden": w_out_hidden, "w_final": w_final}
        static_rows = padded(grid_static.T)
        force = [jnp.concatenate([padded(forcing[:, s, :].T), static_rows], axis=0) for s in range(2)]

        def process(h):
            h = exchange(h).reshape(Q, RLOC, LAT)
            h = processor(h, edge_lat, 0, w_edge_in, w_edge_out, w_node_in, w_node_out)
            return exchange(h.reshape(ring, 2, RLOC, LAT))

        now = x_cur.T
        grid_lat, h = grid_call({"cur": now, "prev": x_prev.T, "force": force[0], "g2m": lat, "mesh": lat}, enc_w, False, True, "encode")
        h = process(h)
        x_next, grid_lat, h = grid_call({"cur": now, "h_in": h, "grid_cur": grid_lat, "m2g": lat, "force": force[1], "g2m": lat, "mesh": lat}, {**dec_w, **enc_w}, True, True, "decode_encode")
        h = process(h)
        x_after, = grid_call({"cur": x_next, "h_in": h, "grid_cur": grid_lat, "m2g": lat}, dec_w, True, False, "decode")
        return x_next.T, x_after.T

    in_specs = (row_spec, row_spec, edge_spec, row_spec, row_spec, row_spec, row_spec, edge_spec, whole) + (whole,) * 11
    return jax.shard_map(local_run, mesh=mesh, in_specs=in_specs, out_specs=(row_spec, row_spec), check_vma=False)
```

```python
import functools

import jax
import jax.numpy as jnp
from jax import lax
from jax.experimental import pallas as pl
from jax.experimental.pallas import tpu as pltpu
from jax.sharding import PartitionSpec as P

F32 = jnp.float32
BF16 = jnp.bfloat16
LAT = 512
VARS = 83
LANES = 128
CELLS = 128
RATIO = 4
ROWS = CELLS * RATIO
SUB = 2
Q = 8
RLOC = 128
NODES = Q * RLOC
OFFS = 6
LAYERS = 12
TILE = 256
CHUNK = 512
VMEM_LIMIT = 60 * 1024 * 1024


def mm(lhs, rhs):
    return jnp.dot(lhs, rhs, preferred_element_type=F32)


def silu_twice(x):
    return (x + x * jnp.tanh(x)).astype(BF16)


def half_norm(y):
    centred = y - jnp.sum(y, axis=-1, keepdims=True) * (1.0 / LAT)
    spread = jnp.sum(centred * centred, axis=-1, keepdims=True)
    return centred * (lax.rsqrt(spread + LAT * 1e-5) * (0.5 * LAT ** 0.5))


def add_to(base, update):
    return (base.astype(F32) + update).astype(BF16)


def mm_features(feats, weight):
    return lax.dot_general(feats, weight, (((0,), (0,)), ((), ())), preferred_element_type=F32)


def embed_kernel(x_ref, w_in_ref, w_out_ref, o_ref):
    halves = [slice(s * ROWS, (s + 1) * ROWS) for s in range(SUB)]
    hid = [silu_twice(mm_features(0.5 * x_ref[:, cols], w_in_ref[0])) for cols in halves]
    upd = [mm(h, w_out_ref[0]) for h in hid]
    for s in range(SUB):
        o_ref[halves[s], :] = half_norm(upd[s]).astype(BF16)


def embed_static(feats, w_in, w_out, first, starts, name):
    depth, rows = feats.shape
    block = SUB * ROWS

    def kind(i):
        return sum((i >= s // block).astype(jnp.int32) for s in starts) if starts else 0

    return pl.pallas_call(
        embed_kernel,
        grid=(rows // block,),
        in_specs=[
            pl.BlockSpec((depth, block), lambda i: (0, i)),
            pl.BlockSpec((1, depth, LAT), lambda i: (kind(i), 0, 0)),
            pl.BlockSpec((1, LAT, LAT), lambda i: (kind(i) + first, 0, 0)),
        ],
        out_specs=pl.BlockSpec((block, LAT), lambda i: (i, 0)),
        out_shape=jax.ShapeDtypeStruct((rows, LAT), BF16),
        compiler_params=pltpu.CompilerParams(vmem_limit_bytes=VMEM_LIMIT),
        cost_estimate=pl.CostEstimate(flops=6 * rows * LAT * LAT, bytes_accessed=2 * rows * LAT, transcendentals=0),
        name=name,
    )(feats, w_in, w_out)


RING = 4


def greet():
    me = lax.axis_index("gp")
    barrier = pltpu.get_barrier_semaphore()
    for hop in range(1, RING):
        pl.semaphore_signal(barrier, inc=1, device_id={"gp": lax.rem(me + hop, RING)}, device_id_type=pl.DeviceIdType.MESH)


def greeted():
    pl.semaphore_wait(pltpu.get_barrier_semaphore(), RING - 1)


class Parcel:

    def __init__(self, peer, src, dst, send_sem, recv_sem):
        self.peer, self.src, self.dst, self.send_sem, self.recv_sem = peer, src, dst, send_sem, recv_sem

    def remote(self):
        return pltpu.make_async_remote_copy(src_ref=self.src, dst_ref=self.dst, send_sem=self.send_sem, recv_sem=self.recv_sem, device_id={"gp": self.peer}, device_id_type=pl.DeviceIdType.MESH)

    def either(self, remote_act, local_act):
        me = lax.axis_index("gp")
        pl.when(self.peer != me)(lambda: getattr(self.remote(), remote_act)())
        if local_act:
            pl.when(self.peer == me)(lambda: getattr(pltpu.make_async_copy(self.src, self.dst, self.send_sem), local_act)())

    def start(self):
        self.either("start", "start")

    def wait_sent(self):
        self.either("wait_send", "wait")

    def wait_arrived(self):
        self.either("wait_recv", None)


def rows_of(sub, size):
    return pl.ds(sub * size, size)


LANE_COLS = [slice(c * LANES, (c + 1) * LANES) for c in range(LAT // LANES)]


def spread(buf, sub, cell_rows):
    for c, col in enumerate(LANE_COLS):
        for k in range(RATIO):
            buf[c, pl.ds(sub * ROWS + k, CELLS, stride=RATIO), :] = cell_rows[:, col]
    return jnp.concatenate([buf[c, rows_of(sub, ROWS), :] for c in range(len(LANE_COLS))], axis=1)


def gather_sum(buf, sub, node_rows):
    for c, col in enumerate(LANE_COLS):
        buf[c, rows_of(sub, ROWS), :] = node_rows[:, col]
    sums = []
    for c in range(len(LANE_COLS)):
        parts = [buf[c, pl.ds(sub * ROWS + k, CELLS, stride=RATIO), :] for k in range(RATIO)]
        sums.append(parts[0] + parts[1] + parts[2] + parts[3])
    return jnp.concatenate(sums, axis=1).astype(BF16)


FEAT_CUR = 88
FEAT_FORCE = 176
FEAT_ROWS = 192


def grid_kernel(names, decode, encode, *refs):
    r = dict(zip(names, refs))
    mean, std, diff_mean, diff_std = (r["stats"][:, i:i + 1] for i in range(4))
    subs = range(SUB)
    cols = [slice(s * ROWS, (s + 1) * ROWS) for s in subs]
    cur = [r["cur"][:, c] for c in cols]
    if decode:
        grid_cur = [r["grid_cur"][rows_of(s, ROWS), :] for s in subs]
        pre = []
        for s in subs:
            send = mm(r["h_in"][s, 0], r["wl"][LAT:2 * LAT, :])
            both = mm(r["m2g"][rows_of(s, ROWS), :], r["wl"][:LAT, :]) + mm(grid_cur[s], r["wl"][2 * LAT:, :])
            pre.append(both + spread(r["buf_send"], s, send))
        hid = [silu_twice(p) for p in pre]
        upd = [mm(h, r["wl_out"][...]) for h in hid]
        edge = [add_to(r["m2g"][rows_of(s, ROWS), :], half_norm(upd[s])) for s in subs]
        pre = [mm(grid_cur[s], r["wl_node"][:LAT, :]) + mm(edge[s], r["wl_node"][LAT:, :]) for s in subs]
        hid = [silu_twice(p) for p in pre]
        upd = [mm(h, r["wl_node_out"][...]) for h in hid]
        out = [add_to(grid_cur[s], half_norm(upd[s])) for s in subs]
        hid = [silu_twice(mm(o, r["w_hidden"][...])) for o in out]
        pred = [mm(h, r["w_final"][...]).T[:VARS] for h in hid]
        nxt = [cur[s] + diff_std * pred[s] + diff_mean for s in subs]
        for s in subs:
            r["next"][:, cols[s]] = nxt[s]
    if encode:
        if decode:
            first, second = cur, nxt
        else:
            first, second = [r["prev"][:, c] for c in cols], cur
        table = r["buf_feat"]
        feats = []
        for s in subs:
            table[VARS - 3:FEAT_CUR, cols[s]] = jnp.zeros((8, ROWS), F32)
            table[FEAT_FORCE - 8:FEAT_FORCE, cols[s]] = jnp.zeros((8, ROWS), F32)
            table[:VARS, cols[s]] = (first[s] - mean) / std
            table[FEAT_CUR:FEAT_CUR + VARS, cols[s]] = (second[s] - mean) / std
            table[FEAT_FORCE:, cols[s]] = r["force"][:, cols[s]]
            feats.append(0.5 * table[:, cols[s]].astype(BF16))
        hid = [silu_twice(mm_features(f, r["w_grid"][...])) for f in feats]
        v = [half_norm(mm(h, r["w_grid_out"][...])).astype(BF16) for h in hid]
        pre = []
        for s in subs:
            recv = mm(r["mesh"][rows_of(s, CELLS), :], r["wf"][2 * LAT:, :])
            both = mm(r["g2m"][rows_of(s, ROWS), :], r["wf"][:LAT, :]) + mm(v[s], r["wf"][LAT:2 * LAT, :])
            pre.append(both + spread(r["buf_recv"], s, recv))
        self_hid = [silu_twice(mm(x, r["w_self"][0])) for x in v]
        hid = [silu_twice(p) for p in pre]
        upd = [mm(h, r["wf_out"][...]) for h in hid]
        self_upd = [mm(h, r["w_self"][1]) for h in self_hid]
        total = [gather_sum(r["buf_sum"], s, add_to(r["g2m"][rows_of(s, ROWS), :], half_norm(upd[s])).astype(F32)) for s in subs]
        mesh = [r["mesh"][rows_of(s, CELLS), :] for s in subs]
        pre = [mm(mesh[s], r["wf_node"][:LAT, :]) + mm(total[s], r["wf_node"][LAT:, :]) for s in subs]
        for s in subs:
            r["grid_new"][rows_of(s, ROWS), :] = add_to(v[s], half_norm(self_upd[s]))
        hid = [silu_twice(p) for p in pre]
        upd = [mm(h, r["wf_node_out"][...]) for h in hid]
        step = pl.program_id(0)
        me = lax.axis_index("gp")

        def parcel(tile):
            slot = 2 * me + tile // RING
            return Parcel(tile % RING, r["h_buf"].at[tile], r["h_out"].at[slot], r["send_sem"].at[tile], r["recv_sem"].at[slot])

        for s in subs:
            r["h_buf"][step * SUB + s] = add_to(mesh[s], half_norm(upd[s]))

        @pl.when(step == 0)
        def first_step():
            greet()
            greeted()

        for s in subs:
            parcel(step * SUB + s).start()

        @pl.when(step == pl.num_programs(0) - 1)
        def last_step():
            for tile in range(2 * RING):
                parcel(tile).wait_sent()
            for slot in range(2 * RING):
                Parcel(slot // 2, r["h_buf"].at[slot], r["h_out"].at[slot], r["send_sem"].at[slot], r["recv_sem"].at[slot]).wait_arrived()


def grid_call(arrays, weights, decode, encode, name):
    tiles = arrays["cur"].shape[1] // ROWS
    lead = tiles // 2
    step_rows = SUB * ROWS
    node_spec = pl.BlockSpec((SUB, 1, CELLS, LAT), lambda i: (i % (lead // SUB), i // (lead // SUB), 0, 0))
    special = {
        "h_in": node_spec,
        "grid_cur": pl.BlockSpec((step_rows, LAT), lambda i: (i, 0)),
        "mesh": pl.BlockSpec((SUB * CELLS, LAT), lambda i: (i, 0)),
        "g2m": pl.BlockSpec((step_rows, LAT), lambda i: (i + 1, 0)),
        "m2g": pl.BlockSpec((step_rows, LAT), lambda i: (i + 1 + tiles // SUB, 0)),
    }
    names, specs, operands = [], [], []
    for key, arr in arrays.items():
        names.append(key)
        operands.append(arr)
        specs.append(special.get(key) or pl.BlockSpec((arr.shape[0], step_rows), lambda i: (0, i)))
    for key, arr in weights.items():
        names.append(key)
        if isinstance(arr, tuple):
            arr, layer = arr
            specs.append(pl.BlockSpec((None,) + arr.shape[1:], functools.partial(lambda at, nd, i: (at,) + (0,) * nd, layer, arr.ndim - 1)))
        else:
            specs.append(pl.BlockSpec(arr.shape, functools.partial(lambda nd, i: (0,) * nd, arr.ndim)))
        operands.append(arr)
    out_specs, out_shapes, scratch = [], [], []
    wide = pltpu.VMEM((len(LANE_COLS), step_rows, LANES), F32)
    if decode:
        names.append("next")
        out_specs.append(pl.BlockSpec((VARS, step_rows), lambda i: (0, i)))
        out_shapes.append(jax.ShapeDtypeStruct((VARS, tiles * ROWS), F32))
    if encode:
        names += ["grid_new", "h_out"]
        out_specs += [pl.BlockSpec((step_rows, LAT), lambda i: (i, 0)), pl.BlockSpec(memory_space=pltpu.HBM)]
        out_shapes += [jax.ShapeDtypeStruct((tiles * ROWS, LAT), BF16), jax.ShapeDtypeStruct((Q, RLOC, LAT), BF16)]
    if decode:
        names.append("buf_send")
        scratch.append(wide)
    if encode:
        names += ["buf_recv", "buf_sum", "buf_feat", "h_buf", "send_sem", "recv_sem"]
        scratch += [wide, wide, pltpu.VMEM((FEAT_ROWS, step_rows), F32), pltpu.VMEM((tiles, CELLS, LAT), BF16)]
        scratch += [pltpu.SemaphoreType.DMA((tiles,))] * 2
    params = dict(collective_id=1 + decode, has_side_effects=True) if encode else {}
    return pl.pallas_call(
        functools.partial(grid_kernel, tuple(names), decode, encode),
        grid=(tiles // SUB,),
        in_specs=specs,
        out_specs=out_specs,
        out_shape=out_shapes,
        scratch_shapes=scratch,
        compiler_params=pltpu.CompilerParams(vmem_limit_bytes=VMEM_LIMIT, **params),
        cost_estimate=pl.CostEstimate(flops=2 * 7 * tiles * ROWS * LAT * LAT * (decode + encode), bytes_accessed=2 ** 24, transcendentals=0),
        name=name,
    )(*operands)


def proc_kernel(first_edge, h_in, lat, w_ei, w_eo, w_ni, w_no, h_out, edge, mesh, proj, recv, total, turn, out_buf, halo, b_ei, b_eo, b_ni, b_no, w_sem, e_sem, s_sem, r_sem, o_send, o_recv):
    me = lax.axis_index("gp")
    right = lax.rem(me + 1, RING)
    left = lax.rem(me + RING - 1, RING)

    def edge_weights(layer):
        slot = lax.rem(layer, 2)
        return [pltpu.make_async_copy(src.at[layer], dst.at[slot], w_sem.at[slot, i]) for i, (src, dst) in enumerate(((w_ei, b_ei), (w_eo, b_eo)))]

    def node_weights(layer):
        slot = lax.rem(layer, 2)
        return [pltpu.make_async_copy(src.at[layer], dst.at[slot], w_sem.at[slot, 2 + i]) for i, (src, dst) in enumerate(((w_ni, b_ni), (w_no, b_no)))]

    def start_all(copies):
        for copy in copies:
            copy.start()

    def wait_all(copies):
        for copy in copies:
            copy.wait()

    edge_copies = [pltpu.make_async_copy(lat.at[pl.ds(first_edge + k * NODES, NODES)], edge.at[k], e_sem.at[k]) for k in range(OFFS)]
    start_all(edge_weights(1) + node_weights(1) + edge_copies)

    greet()
    for c, col in enumerate(LANE_COLS):
        for q in range(Q):
            turn[c, pl.ds(q, RLOC, stride=Q), :] = h_in[q, :, col].astype(F32)
    for c, col in enumerate(LANE_COLS):
        mesh[:, col] = turn[c].astype(BF16)
    greeted()
    wait_all(edge_weights(1) + node_weights(1))
    total[...] = jnp.zeros_like(total)
    for c in range(2):
        rows = pl.ds(c * 512, 512)
        proj[1, pl.ds(8 + c * 512, 512), :] = mm(mesh[rows, :], b_ei[1, LAT:2 * LAT, :])
        recv[1, rows, :] = mm(mesh[rows, :], b_ei[1, 2 * LAT:, :])
    wait_all(edge_copies)

    def order(j):
        return lax.rem(j + 1, 3) + 2 * (j // 3)

    def node_rows(t):
        return pl.ds(pl.multiple_of(t * TILE, TILE), TILE)

    def tile_step(l, j):
        slot = lax.rem(l, 2)
        start = pl.multiple_of(order(j) * TILE, TILE)
        rows = pl.ds(start, TILE)
        first = j == 0
        first_ever = jnp.logical_and(first, l == 1)
        before = node_rows(order(lax.rem(j + 3, 4)))
        node_slot = lax.rem(l + jnp.where(jnp.logical_and(first, l > 1), 1, 0), 2)
        next_slot = lax.rem(l + jnp.where(first, 0, 1), 2)
        nodes = mesh[before, :]
        sums = total[before, :]

        at_recv = recv[slot, rows, :]
        here = proj[slot, pl.ds(start + 8, TILE), :].reshape(TILE // Q, Q, LAT)

        def sender(k):
            if k == 0:
                return proj[slot, pl.ds(start + 16, TILE), :]
            if k == 1:
                return proj[slot, rows, :]
            shift = {2: Q - 1, 3: 1, 4: Q - 2, 5: 2}[k]
            return pltpu.roll(here, shift, 1).reshape(TILE, LAT)

        w_first = b_ei[slot, :LAT, :]
        w_second = b_eo[slot]
        chunks = OFFS * TILE // CHUNK
        per = CHUNK // TILE
        old, hid, upd = {}, {}, {}
        acc = [None]

        def stage_a(c):
            pair = edge[per * c:per * c + per, rows, :].reshape(CHUNK, LAT)
            old[c] = pair
            terms = jnp.concatenate([sender(per * c + i) + at_recv for i in range(per)], axis=0)
            hid[c] = silu_twice(mm(pair, w_first) + terms)

        def stage_b(c):
            upd[c] = mm(hid[c], w_second)

        def stage_c(c):
            new = add_to(old[c], half_norm(upd[c]))
            edge[per * c:per * c + per, rows, :] = new.reshape(per, TILE, LAT)
            wide = new.astype(F32)
            for i in range(per):
                part = wide[i * TILE:(i + 1) * TILE]
                acc[0] = part if acc[0] is None else acc[0] + part

        stage_a(0)
        stage_a(1)
        node_hid = silu_twice(mm(nodes, b_ni[node_slot, :LAT, :]) + mm(sums, b_ni[node_slot, LAT:, :]))
        stage_b(0)
        stage_a(2)
        node_upd = mm(node_hid, b_no[node_slot])
        stage_b(1)
        stage_c(0)
        stage_b(2)
        node_new = add_to(nodes, half_norm(node_upd))
        node_new = jnp.where(first_ever, nodes, node_new)
        send_next = mm(node_new, b_ei[next_slot, LAT:2 * LAT, :])
        recv_next = mm(node_new, b_ei[next_slot, 2 * LAT:, :])
        stage_c(1)
        stage_c(2)
        total[rows, :] = acc[0].astype(BF16)
        mesh[before, :] = node_new
        proj[next_slot, pl.ds(order(lax.rem(j + 3, 4)) * TILE + 8, TILE), :] = send_next
        recv[next_slot, before, :] = recv_next

    def last_nodes(t):
        rows = node_rows(t)
        slot = LAYERS % 2
        hid = silu_twice(mm(mesh[rows, :], b_ni[slot, :LAT, :]) + mm(total[rows, :], b_ni[slot, LAT:, :]))
        mesh[rows, :] = add_to(mesh[rows, :], half_norm(mm(hid, b_no[slot])))

    tile_r = TILE // Q

    def parcels(t, sender):
        rows = pl.ds(pl.multiple_of(t * tile_r, tile_r), tile_r)
        made = []
        for q in range(Q):
            if sender:
                slot = 2 * me + q % 2
                made.append(Parcel(q // 2, out_buf.at[q, rows], h_out.at[me, q % 2, rows], o_send.at[t, q], o_recv.at[t, slot]))
            else:
                made.append(Parcel(q // 2, out_buf.at[q, rows], h_out.at[q // 2, q % 2, rows], o_send.at[t, q], o_recv.at[t, q]))
        return made

    def hand_over(t):
        start = pl.multiple_of(t * TILE, TILE)
        rows = pl.ds(start, TILE)
        for c, col in enumerate(LANE_COLS):
            turn[c, rows, :] = mesh[rows, col].astype(F32)
        for c, col in enumerate(LANE_COLS):
            for q in range(Q):
                out_buf[q, pl.ds(pl.multiple_of(t * tile_r, tile_r), tile_r), col] = turn[c, pl.ds(start + q, tile_r, stride=Q), :].astype(BF16)
        for parcel in parcels(t, True):
            parcel.start()

    def halo_copy(slot, side):
        first, peer = ((NODES, right), (8, left))[side]
        return pltpu.make_async_remote_copy(
            src_ref=proj.at[slot, pl.ds(first, 8)],
            dst_ref=halo.at[slot, side],
            send_sem=s_sem.at[side],
            recv_sem=r_sem.at[slot, side],
            device_id={"gp": peer},
            device_id_type=pl.DeviceIdType.MESH)

    def layer(l, carry):
        slot = lax.rem(l, 2)
        start_all(edge_weights(l + 1))
        halo_copy(slot, 1).start()

        def body(j, carry):
            @pl.when(j == 1)
            def after_first():
                halo_copy(slot, 0).start()
                start_all(node_weights(l + 1))
                wait_all(edge_weights(l + 1))

            @pl.when(j == 2)
            def border_below():
                halo_copy(slot, 0).wait_recv()
                below = halo[slot, 0]
                proj[slot, 0:8, :] = jnp.where(me == 0, pltpu.roll(below, 1, 0), below)

            @pl.when(j == 3)
            def border_above():
                halo_copy(slot, 1).wait_recv()
                above = halo[slot, 1]
                proj[slot, 8 + NODES:16 + NODES, :] = jnp.where(me == RING - 1, pltpu.roll(above, Q - 1, 0), above)

            tile_step(l, j)

            @pl.when(jnp.logical_and(l == LAYERS, j > 0))
            def leave():
                hand_over(order(j - 1))

            return carry

        lax.fori_loop(0, NODES // TILE, body, 0)
        halo_copy(slot, 0).wait_send()
        halo_copy(slot, 1).wait_send()
        wait_all(node_weights(l + 1))
        return carry

    lax.fori_loop(1, LAYERS + 1, layer, 0)
    last_nodes(order(3))
    hand_over(order(3))

    def settle(t, carry):
        for parcel in parcels(t, True):
            parcel.wait_sent()
        for parcel in parcels(t, False):
            parcel.wait_arrived()
        return carry

    lax.fori_loop(0, NODES // TILE, settle, 0)


def processor(h_in, lat, first_edge, w_edge_in, w_edge_out, w_node_in, w_node_out):
    hbm = pl.BlockSpec(memory_space=pl.ANY)
    vmem = pl.BlockSpec(memory_space=pltpu.VMEM)
    rows = NODES * (OFFS * 2 + 8)
    return pl.pallas_call(
        functools.partial(proc_kernel, first_edge),
        in_specs=[vmem, hbm, hbm, hbm, hbm, hbm],
        out_specs=pl.BlockSpec(memory_space=pltpu.HBM),
        out_shape=jax.ShapeDtypeStruct((RING, 2, RLOC, LAT), BF16),
        scratch_shapes=[
            pltpu.VMEM((OFFS, NODES, LAT), BF16),
            pltpu.VMEM((NODES, LAT), BF16),
            pltpu.VMEM((2, NODES + 16, LAT), F32),
            pltpu.VMEM((2, NODES, LAT), F32),
            pltpu.VMEM((NODES, LAT), BF16),
            pltpu.VMEM((LAT // LANES, NODES, LANES), F32),
            pltpu.VMEM((Q, RLOC, LAT), BF16),
            pltpu.VMEM((2, 2, 8, LAT), F32),
            pltpu.VMEM((2, 3 * LAT, LAT), BF16),
            pltpu.VMEM((2, LAT, LAT), BF16),
            pltpu.VMEM((2, 2 * LAT, LAT), BF16),
            pltpu.VMEM((2, LAT, LAT), BF16),
            pltpu.SemaphoreType.DMA((2, 4)),
            pltpu.SemaphoreType.DMA((OFFS,)),
            pltpu.SemaphoreType.DMA((2,)),
            pltpu.SemaphoreType.DMA((2, 2)),
            pltpu.SemaphoreType.DMA((NODES // TILE, Q)),
            pltpu.SemaphoreType.DMA((NODES // TILE, Q)),
        ],
        compiler_params=pltpu.CompilerParams(collective_id=0, has_side_effects=True, vmem_limit_bytes=VMEM_LIMIT),
        cost_estimate=pl.CostEstimate(flops=2 * LAYERS * rows * LAT * LAT, bytes_accessed=60 * 2 ** 20, transcendentals=0),
        name="processor",
    )(h_in, lat, w_edge_in, w_edge_out, w_node_in, w_node_out)


def solution(mesh):
    ring = mesh.shape["gp"]
    row_spec = P(("dp", "gp"))
    edge_spec = P(("dp", "gp"), None, None)
    whole = P()

    def exchange(x):
        return lax.all_to_all(x, "gp", 0, 0)

    def local_run(x_prev, x_cur, forcing, grid_static, g2m_feat, m2g_feat, mesh_feat, mesh_edge_feat, norm_stats, w_grid_in, w_mesh_in, w_eemb_in, w_embed_out, w_edge_in, w_edge_out, w_node_in, w_node_out, w_grid_self, w_out_hidden, w_out_final):
        grid_dev = x_prev.shape[0]
        mesh_dev = mesh_feat.shape[0]
        half = mesh_dev // 2
        deep = 8

        def padded(x):
            return jnp.pad(x, ((0, deep - x.shape[0]), (0, 0)))

        edges = mesh_edge_feat.astype(BF16).transpose(1, 2, 0).reshape(OFFS * 4, 2, ring, RLOC).transpose(2, 0, 1, 3)
        edges = exchange(edges)
        edges = edges.reshape(ring, OFFS, 4, 2, RLOC).transpose(2, 1, 4, 0, 3).reshape(4, OFFS * RLOC, Q)
        edges = padded(jnp.roll(edges, -1, axis=2).reshape(4, OFFS * NODES))
        node_rows = mesh_feat.astype(BF16).T
        g2m_rows = g2m_feat.astype(BF16).T
        head = jnp.concatenate([node_rows[:, :half]] + [g2m_rows[:, k * half:(k + 1) * half] for k in range(RATIO)], axis=0)
        head = lax.ppermute(head, "gp", [(s, (s - 1) % ring) for s in range(ring)])
        node_rows = padded(jnp.concatenate([node_rows[:, half:], head[:3]], axis=1))
        g2m_rows = padded(jnp.concatenate([g2m_rows[:, RATIO * half:]] + [head[3 + 4 * k:7 + 4 * k] for k in range(RATIO)], axis=1))
        feats = jnp.concatenate([node_rows, g2m_rows, padded(m2g_feat.astype(BF16).T)], axis=1)
        lat = embed_static(feats, jnp.stack([padded(w_mesh_in), padded(w_eemb_in[0]), padded(w_eemb_in[1])]), w_embed_out, 1, (mesh_dev, mesh_dev + grid_dev), "embed")
        edge_lat = embed_static(edges, padded(w_eemb_in[2])[None], w_embed_out, 4, (), "embed_edges")

        w_grid = jnp.concatenate([
            jnp.pad(w_grid_in[:VARS], ((0, FEAT_CUR - VARS), (0, 0))),
            jnp.pad(w_grid_in[VARS:2 * VARS], ((0, FEAT_CUR - VARS), (0, 0))),
            padded(w_grid_in[2 * VARS:2 * VARS + 5]), padded(w_grid_in[2 * VARS + 5:])], axis=0)
        w_final = jnp.pad(w_out_final, ((0, 0), (0, LANES - VARS)))
        last = w_edge_in.shape[0] - 1
        stats = norm_stats.T
        enc_w = {"stats": stats, "w_grid": w_grid, "w_grid_out": (w_embed_out, 0), "wf": (w_edge_in, 0), "wf_out": (w_edge_out, 0), "wf_node": (w_node_in, 0), "wf_node_out": (w_node_out, 0), "w_self": w_grid_self}
        dec_w = {"stats": stats, "wl": (w_edge_in, last), "wl_out": (w_edge_out, last), "wl_node": (w_node_in, last), "wl_node_out": (w_node_out, last), "w_hidden": w_out_hidden, "w_final": w_final}
        static_rows = padded(grid_static.T)
        force = [jnp.concatenate([padded(forcing[:, s, :].T), static_rows], axis=0) for s in range(2)]

        def process(h):
            return processor(h, edge_lat, 0, w_edge_in, w_edge_out, w_node_in, w_node_out)

        now = x_cur.T
        grid_lat, h = grid_call({"cur": now, "prev": x_prev.T, "force": force[0], "g2m": lat, "mesh": lat}, enc_w, False, True, "encode")
        h = process(h)
        x_next, grid_lat, h = grid_call({"cur": now, "h_in": h, "grid_cur": grid_lat, "m2g": lat, "force": force[1], "g2m": lat, "mesh": lat}, {**dec_w, **enc_w}, True, True, "decode_encode")
        h = process(h)
        x_after, = grid_call({"cur": x_next, "h_in": h, "grid_cur": grid_lat, "m2g": lat}, dec_w, True, False, "decode")
        return x_next.T, x_after.T

    in_specs = (row_spec, row_spec, edge_spec, row_spec, row_spec, row_spec, row_spec, edge_spec, whole) + (whole,) * 11
    return jax.shard_map(local_run, mesh=mesh, in_specs=in_specs, out_specs=(row_spec, row_spec), check_vma=False)
```

```python
import functools

import jax
import jax.numpy as jnp
from jax import lax
from jax.experimental import pallas as pl
from jax.experimental.pallas import tpu as pltpu
from jax.sharding import PartitionSpec as P

F32 = jnp.float32
BF16 = jnp.bfloat16
LAT = 512
VARS = 83
LANES = 128
CELLS = 128
RATIO = 4
ROWS = CELLS * RATIO
SUB = 2
Q = 8
RLOC = 128
NODES = Q * RLOC
OFFS = 6
LAYERS = 12
TILE = 256
CHUNK = 512
VMEM_LIMIT = 60 * 1024 * 1024


def mm(lhs, rhs):
    return jnp.dot(lhs, rhs, preferred_element_type=F32)


def silu_twice(x):
    return (x + x * jnp.tanh(x)).astype(BF16)


def half_norm(y):
    centred = y - jnp.sum(y, axis=-1, keepdims=True) * (1.0 / LAT)
    spread = jnp.sum(centred * centred, axis=-1, keepdims=True)
    return centred * (lax.rsqrt(spread + LAT * 1e-5) * (0.5 * LAT ** 0.5))


def add_to(base, update):
    return (base.astype(F32) + update).astype(BF16)


def mm_features(feats, weight):
    return lax.dot_general(feats, weight, (((0,), (0,)), ((), ())), preferred_element_type=F32)


def embed_kernel(x_ref, w_in_ref, w_out_ref, o_ref):
    halves = [slice(s * ROWS, (s + 1) * ROWS) for s in range(SUB)]
    hid = [silu_twice(mm_features(0.5 * x_ref[:, cols], w_in_ref[0])) for cols in halves]
    upd = [mm(h, w_out_ref[0]) for h in hid]
    for s in range(SUB):
        o_ref[halves[s], :] = half_norm(upd[s]).astype(BF16)


def embed_static(feats, w_in, w_out, first, starts, name):
    depth, rows = feats.shape
    block = SUB * ROWS

    def kind(i):
        return sum((i >= s // block).astype(jnp.int32) for s in starts) if starts else 0

    return pl.pallas_call(
        embed_kernel,
        grid=(rows // block,),
        in_specs=[
            pl.BlockSpec((depth, block), lambda i: (0, i)),
            pl.BlockSpec((1, depth, LAT), lambda i: (kind(i), 0, 0)),
            pl.BlockSpec((1, LAT, LAT), lambda i: (kind(i) + first, 0, 0)),
        ],
        out_specs=pl.BlockSpec((block, LAT), lambda i: (i, 0)),
        out_shape=jax.ShapeDtypeStruct((rows, LAT), BF16),
        compiler_params=pltpu.CompilerParams(vmem_limit_bytes=VMEM_LIMIT),
        cost_estimate=pl.CostEstimate(flops=6 * rows * LAT * LAT, bytes_accessed=2 * rows * LAT, transcendentals=0),
        name=name,
    )(feats, w_in, w_out)


RING = 4


def greet():
    me = lax.axis_index("gp")
    barrier = pltpu.get_barrier_semaphore()
    for hop in range(1, RING):
        pl.semaphore_signal(barrier, inc=1, device_id={"gp": lax.rem(me + hop, RING)}, device_id_type=pl.DeviceIdType.MESH)


def greeted():
    pl.semaphore_wait(pltpu.get_barrier_semaphore(), RING - 1)


class Parcel:

    def __init__(self, peer, src, dst, send_sem, recv_sem):
        self.peer, self.src, self.dst, self.send_sem, self.recv_sem = peer, src, dst, send_sem, recv_sem

    def remote(self):
        return pltpu.make_async_remote_copy(src_ref=self.src, dst_ref=self.dst, send_sem=self.send_sem, recv_sem=self.recv_sem, device_id={"gp": self.peer}, device_id_type=pl.DeviceIdType.MESH)

    def either(self, remote_act, local_act):
        me = lax.axis_index("gp")
        pl.when(self.peer != me)(lambda: getattr(self.remote(), remote_act)())
        if local_act:
            pl.when(self.peer == me)(lambda: getattr(pltpu.make_async_copy(self.src, self.dst, self.send_sem), local_act)())

    def start(self):
        self.either("start", "start")

    def wait_sent(self):
        self.either("wait_send", "wait")

    def wait_arrived(self):
        self.either("wait_recv", None)


def pair_of(i):
    chip = lax.axis_index("gp") // 2
    return 2 * lax.rem(i, 2) + (1 - chip) + (i // 2) * (2 * chip - 1)


def rows_of(sub, size):
    return pl.ds(sub * size, size)


LANE_COLS = [slice(c * LANES, (c + 1) * LANES) for c in range(LAT // LANES)]


def spread(buf, sub, cell_rows):
    for c, col in enumerate(LANE_COLS):
        for k in range(RATIO):
            buf[c, pl.ds(sub * ROWS + k, CELLS, stride=RATIO), :] = cell_rows[:, col]
    return jnp.concatenate([buf[c, rows_of(sub, ROWS), :] for c in range(len(LANE_COLS))], axis=1)


def gather_sum(buf, sub, node_rows):
    for c, col in enumerate(LANE_COLS):
        buf[c, rows_of(sub, ROWS), :] = node_rows[:, col]
    sums = []
    for c in range(len(LANE_COLS)):
        parts = [buf[c, pl.ds(sub * ROWS + k, CELLS, stride=RATIO), :] for k in range(RATIO)]
        sums.append(parts[0] + parts[1] + parts[2] + parts[3])
    return jnp.concatenate(sums, axis=1).astype(BF16)


FEAT_CUR = 88
FEAT_FORCE = 176
FEAT_ROWS = 192


def grid_kernel(names, decode, encode, *refs):
    r = dict(zip(names, refs))
    mean, std, diff_mean, diff_std = (r["stats"][:, i:i + 1] for i in range(4))
    subs = range(SUB)
    cols = [slice(s * ROWS, (s + 1) * ROWS) for s in subs]
    cur = [r["cur"][:, c] for c in cols]
    if decode:
        grid_cur = [r["grid_cur"][rows_of(s, ROWS), :] for s in subs]
        pre = []
        for s in subs:
            send = mm(r["h_in"][s, 0], r["wl"][LAT:2 * LAT, :])
            both = mm(r["m2g"][rows_of(s, ROWS), :], r["wl"][:LAT, :]) + mm(grid_cur[s], r["wl"][2 * LAT:, :])
            pre.append(both + spread(r["buf_send"], s, send))
        hid = [silu_twice(p) for p in pre]
        upd = [mm(h, r["wl_out"][...]) for h in hid]
        edge = [add_to(r["m2g"][rows_of(s, ROWS), :], half_norm(upd[s])) for s in subs]
        pre = [mm(grid_cur[s], r["wl_node"][:LAT, :]) + mm(edge[s], r["wl_node"][LAT:, :]) for s in subs]
        hid = [silu_twice(p) for p in pre]
        upd = [mm(h, r["wl_node_out"][...]) for h in hid]
        out = [add_to(grid_cur[s], half_norm(upd[s])) for s in subs]
        hid = [silu_twice(mm(o, r["w_hidden"][...])) for o in out]
        pred = [mm(h, r["w_final"][...]).T[:VARS] for h in hid]
        nxt = [cur[s] + diff_std * pred[s] + diff_mean for s in subs]
        for s in subs:
            r["next"][:, cols[s]] = nxt[s]
    if encode:
        if decode:
            first, second = cur, nxt
        else:
            first, second = [r["prev"][:, c] for c in cols], cur
        table = r["buf_feat"]
        feats = []
        for s in subs:
            table[VARS - 3:FEAT_CUR, cols[s]] = jnp.zeros((8, ROWS), F32)
            table[FEAT_FORCE - 8:FEAT_FORCE, cols[s]] = jnp.zeros((8, ROWS), F32)
            table[:VARS, cols[s]] = (first[s] - mean) / std
            table[FEAT_CUR:FEAT_CUR + VARS, cols[s]] = (second[s] - mean) / std
            table[FEAT_FORCE:, cols[s]] = r["force"][:, cols[s]]
            feats.append(0.5 * table[:, cols[s]].astype(BF16))
        hid = [silu_twice(mm_features(f, r["w_grid"][...])) for f in feats]
        v = [half_norm(mm(h, r["w_grid_out"][...])).astype(BF16) for h in hid]
        pre = []
        for s in subs:
            recv = mm(r["mesh"][rows_of(s, CELLS), :], r["wf"][2 * LAT:, :])
            both = mm(r["g2m"][rows_of(s, ROWS), :], r["wf"][:LAT, :]) + mm(v[s], r["wf"][LAT:2 * LAT, :])
            pre.append(both + spread(r["buf_recv"], s, recv))
        self_hid = [silu_twice(mm(x, r["w_self"][0])) for x in v]
        hid = [silu_twice(p) for p in pre]
        upd = [mm(h, r["wf_out"][...]) for h in hid]
        self_upd = [mm(h, r["w_self"][1]) for h in self_hid]
        total = [gather_sum(r["buf_sum"], s, add_to(r["g2m"][rows_of(s, ROWS), :], half_norm(upd[s])).astype(F32)) for s in subs]
        mesh = [r["mesh"][rows_of(s, CELLS), :] for s in subs]
        pre = [mm(mesh[s], r["wf_node"][:LAT, :]) + mm(total[s], r["wf_node"][LAT:, :]) for s in subs]
        for s in subs:
            r["grid_new"][rows_of(s, ROWS), :] = add_to(v[s], half_norm(self_upd[s]))
        hid = [silu_twice(p) for p in pre]
        upd = [mm(h, r["wf_node_out"][...]) for h in hid]
        step = pl.program_id(0)
        pair = pair_of(step)
        me = lax.axis_index("gp")

        def parcel(tile):
            slot = 2 * me + tile // RING
            return Parcel(tile % RING, r["h_buf"].at[tile], r["h_out"].at[slot], r["send_sem"].at[tile], r["recv_sem"].at[slot])

        for s in subs:
            r["h_buf"][pair * SUB + s] = add_to(mesh[s], half_norm(upd[s]))

        @pl.when(step == 0)
        def first_step():
            greet()
            greeted()

        for s in subs:
            parcel(pair * SUB + s).start()

        @pl.when(step == pl.num_programs(0) - 1)
        def last_step():
            for tile in range(2 * RING):
                parcel(tile).wait_sent()
            for slot in range(2 * RING):
                Parcel(slot // 2, r["h_buf"].at[slot], r["h_out"].at[slot], r["send_sem"].at[slot], r["recv_sem"].at[slot]).wait_arrived()


def grid_call(arrays, weights, decode, encode, name):
    tiles = arrays["cur"].shape[1] // ROWS
    lead = tiles // 2
    step_rows = SUB * ROWS
    special = {
        "h_in": pl.BlockSpec((SUB, 1, CELLS, LAT), lambda i: (pair_of(i) % (lead // SUB), pair_of(i) // (lead // SUB), 0, 0)),
        "grid_cur": pl.BlockSpec((step_rows, LAT), lambda i: (pair_of(i), 0)),
        "mesh": pl.BlockSpec((SUB * CELLS, LAT), lambda i: (pair_of(i), 0)),
        "g2m": pl.BlockSpec((step_rows, LAT), lambda i: (pair_of(i) + 1, 0)),
        "m2g": pl.BlockSpec((step_rows, LAT), lambda i: (pair_of(i) + 1 + tiles // SUB, 0)),
    }
    names, specs, operands = [], [], []
    for key, arr in arrays.items():
        names.append(key)
        operands.append(arr)
        specs.append(special.get(key) or pl.BlockSpec((arr.shape[0], step_rows), lambda i: (0, pair_of(i))))
    for key, arr in weights.items():
        names.append(key)
        if isinstance(arr, tuple):
            arr, layer = arr
            specs.append(pl.BlockSpec((None,) + arr.shape[1:], functools.partial(lambda at, nd, i: (at,) + (0,) * nd, layer, arr.ndim - 1)))
        else:
            specs.append(pl.BlockSpec(arr.shape, functools.partial(lambda nd, i: (0,) * nd, arr.ndim)))
        operands.append(arr)
    out_specs, out_shapes, scratch = [], [], []
    wide = pltpu.VMEM((len(LANE_COLS), step_rows, LANES), F32)
    if decode:
        names.append("next")
        out_specs.append(pl.BlockSpec((VARS, step_rows), lambda i: (0, pair_of(i))))
        out_shapes.append(jax.ShapeDtypeStruct((VARS, tiles * ROWS), F32))
    if encode:
        names += ["grid_new", "h_out"]
        out_specs += [pl.BlockSpec((step_rows, LAT), lambda i: (pair_of(i), 0)), pl.BlockSpec(memory_space=pltpu.HBM)]
        out_shapes += [jax.ShapeDtypeStruct((tiles * ROWS, LAT), BF16), jax.ShapeDtypeStruct((Q, RLOC, LAT), BF16)]
    if decode:
        names.append("buf_send")
        scratch.append(wide)
    if encode:
        names += ["buf_recv", "buf_sum", "buf_feat", "h_buf", "send_sem", "recv_sem"]
        scratch += [wide, wide, pltpu.VMEM((FEAT_ROWS, step_rows), F32), pltpu.VMEM((tiles, CELLS, LAT), BF16)]
        scratch += [pltpu.SemaphoreType.DMA((tiles,))] * 2
    params = dict(collective_id=1 + decode, has_side_effects=True) if encode else {}
    return pl.pallas_call(
        functools.partial(grid_kernel, tuple(names), decode, encode),
        grid=(tiles // SUB,),
        in_specs=specs,
        out_specs=out_specs,
        out_shape=out_shapes,
        scratch_shapes=scratch,
        compiler_params=pltpu.CompilerParams(vmem_limit_bytes=VMEM_LIMIT, **params),
        cost_estimate=pl.CostEstimate(flops=2 * 7 * tiles * ROWS * LAT * LAT * (decode + encode), bytes_accessed=2 ** 24, transcendentals=0),
        name=name,
    )(*operands)


def proc_kernel(first_edge, h_in, lat, w_ei, w_eo, w_ni, w_no, h_out, edge, mesh, proj, recv, total, turn, out_buf, halo, b_ei, b_eo, b_ni, b_no, w_sem, e_sem, s_sem, r_sem, o_send, o_recv):
    me = lax.axis_index("gp")
    right = lax.rem(me + 1, RING)
    left = lax.rem(me + RING - 1, RING)

    def edge_weights(layer):
        slot = lax.rem(layer, 2)
        return [pltpu.make_async_copy(src.at[layer], dst.at[slot], w_sem.at[slot, i]) for i, (src, dst) in enumerate(((w_ei, b_ei), (w_eo, b_eo)))]

    def node_weights(layer):
        slot = lax.rem(layer, 2)
        return [pltpu.make_async_copy(src.at[layer], dst.at[slot], w_sem.at[slot, 2 + i]) for i, (src, dst) in enumerate(((w_ni, b_ni), (w_no, b_no)))]

    def start_all(copies):
        for copy in copies:
            copy.start()

    def wait_all(copies):
        for copy in copies:
            copy.wait()

    edge_copies = [pltpu.make_async_copy(lat.at[pl.ds(first_edge + k * NODES, NODES)], edge.at[k], e_sem.at[k]) for k in range(OFFS)]
    start_all(edge_weights(1) + node_weights(1) + edge_copies)

    greet()
    for c, col in enumerate(LANE_COLS):
        for q in range(Q):
            turn[c, pl.ds(q, RLOC, stride=Q), :] = h_in[q, :, col].astype(F32)
    for c, col in enumerate(LANE_COLS):
        mesh[:, col] = turn[c].astype(BF16)
    greeted()
    wait_all(edge_weights(1) + node_weights(1))
    total[...] = jnp.zeros_like(total)
    for c in range(2):
        rows = pl.ds(c * 512, 512)
        proj[1, pl.ds(8 + c * 512, 512), :] = mm(mesh[rows, :], b_ei[1, LAT:2 * LAT, :])
        recv[1, rows, :] = mm(mesh[rows, :], b_ei[1, 2 * LAT:, :])
    wait_all(edge_copies)

    def order(j):
        return lax.rem(j + 1, 3) + 2 * (j // 3)

    def node_rows(t):
        return pl.ds(pl.multiple_of(t * TILE, TILE), TILE)

    def tile_step(l, j):
        slot = lax.rem(l, 2)
        start = pl.multiple_of(order(j) * TILE, TILE)
        rows = pl.ds(start, TILE)
        first = j == 0
        first_ever = jnp.logical_and(first, l == 1)
        before = node_rows(order(lax.rem(j + 3, 4)))
        node_slot = lax.rem(l + jnp.where(jnp.logical_and(first, l > 1), 1, 0), 2)
        next_slot = lax.rem(l + jnp.where(first, 0, 1), 2)
        nodes = mesh[before, :]
        sums = total[before, :]

        at_recv = recv[slot, rows, :]
        here = proj[slot, pl.ds(start + 8, TILE), :].reshape(TILE // Q, Q, LAT)

        def sender(k):
            if k == 0:
                return proj[slot, pl.ds(start + 16, TILE), :]
            if k == 1:
                return proj[slot, rows, :]
            shift = {2: Q - 1, 3: 1, 4: Q - 2, 5: 2}[k]
            return pltpu.roll(here, shift, 1).reshape(TILE, LAT)

        w_first = b_ei[slot, :LAT, :]
        w_second = b_eo[slot]
        chunks = OFFS * TILE // CHUNK
        per = CHUNK // TILE
        old, hid, upd = {}, {}, {}
        acc = [None]

        def stage_a(c):
            pair = edge[per * c:per * c + per, rows, :].reshape(CHUNK, LAT)
            old[c] = pair
            terms = jnp.concatenate([sender(per * c + i) + at_recv for i in range(per)], axis=0)
            hid[c] = silu_twice(mm(pair, w_first) + terms)

        def stage_b(c):
            upd[c] = mm(hid[c], w_second)

        def stage_c(c):
            new = add_to(old[c], half_norm(upd[c]))
            edge[per * c:per * c + per, rows, :] = new.reshape(per, TILE, LAT)
            wide = new.astype(F32)
            for i in range(per):
                part = wide[i * TILE:(i + 1) * TILE]
                acc[0] = part if acc[0] is None else acc[0] + part

        stage_a(0)
        stage_a(1)
        node_hid = silu_twice(mm(nodes, b_ni[node_slot, :LAT, :]) + mm(sums, b_ni[node_slot, LAT:, :]))
        stage_b(0)
        stage_a(2)
        node_upd = mm(node_hid, b_no[node_slot])
        stage_b(1)
        stage_c(0)
        stage_b(2)
        node_new = add_to(nodes, half_norm(node_upd))
        node_new = jnp.where(first_ever, nodes, node_new)
        send_next = mm(node_new, b_ei[next_slot, LAT:2 * LAT, :])
        recv_next = mm(node_new, b_ei[next_slot, 2 * LAT:, :])
        stage_c(1)
        stage_c(2)
        total[rows, :] = acc[0].astype(BF16)
        mesh[before, :] = node_new
        proj[next_slot, pl.ds(order(lax.rem(j + 3, 4)) * TILE + 8, TILE), :] = send_next
        recv[next_slot, before, :] = recv_next

    def last_nodes(t):
        rows = node_rows(t)
        slot = LAYERS % 2
        hid = silu_twice(mm(mesh[rows, :], b_ni[slot, :LAT, :]) + mm(total[rows, :], b_ni[slot, LAT:, :]))
        mesh[rows, :] = add_to(mesh[rows, :], half_norm(mm(hid, b_no[slot])))

    tile_r = TILE // Q

    def parcels(t, sender):
        rows = pl.ds(pl.multiple_of(t * tile_r, tile_r), tile_r)
        made = []
        for q in range(Q):
            if sender:
                slot = 2 * me + q % 2
                made.append(Parcel(q // 2, out_buf.at[q, rows], h_out.at[me, q % 2, rows], o_send.at[t, q], o_recv.at[t, slot]))
            else:
                made.append(Parcel(q // 2, out_buf.at[q, rows], h_out.at[q // 2, q % 2, rows], o_send.at[t, q], o_recv.at[t, q]))
        return made

    def hand_over(t):
        start = pl.multiple_of(t * TILE, TILE)
        rows = pl.ds(start, TILE)
        for c, col in enumerate(LANE_COLS):
            turn[c, rows, :] = mesh[rows, col].astype(F32)
        for c, col in enumerate(LANE_COLS):
            for q in range(Q):
                out_buf[q, pl.ds(pl.multiple_of(t * tile_r, tile_r), tile_r), col] = turn[c, pl.ds(start + q, tile_r, stride=Q), :].astype(BF16)
        for parcel in parcels(t, True):
            parcel.start()

    def halo_copy(slot, side):
        first, peer = ((NODES, right), (8, left))[side]
        return pltpu.make_async_remote_copy(
            src_ref=proj.at[slot, pl.ds(first, 8)],
            dst_ref=halo.at[slot, side],
            send_sem=s_sem.at[side],
            recv_sem=r_sem.at[slot, side],
            device_id={"gp": peer},
            device_id_type=pl.DeviceIdType.MESH)

    def layer(l, carry):
        slot = lax.rem(l, 2)
        start_all(edge_weights(l + 1))
        halo_copy(slot, 1).start()

        def body(j, carry):
            @pl.when(j == 1)
            def after_first():
                halo_copy(slot, 0).start()
                start_all(node_weights(l + 1))
                wait_all(edge_weights(l + 1))

            @pl.when(j == 2)
            def border_below():
                halo_copy(slot, 0).wait_recv()
                below = halo[slot, 0]
                proj[slot, 0:8, :] = jnp.where(me == 0, pltpu.roll(below, 1, 0), below)

            @pl.when(j == 3)
            def border_above():
                halo_copy(slot, 1).wait_recv()
                above = halo[slot, 1]
                proj[slot, 8 + NODES:16 + NODES, :] = jnp.where(me == RING - 1, pltpu.roll(above, Q - 1, 0), above)

            tile_step(l, j)

            @pl.when(jnp.logical_and(l == LAYERS, j > 0))
            def leave():
                hand_over(order(j - 1))

            return carry

        lax.fori_loop(0, NODES // TILE, body, 0)
        halo_copy(slot, 0).wait_send()
        halo_copy(slot, 1).wait_send()
        wait_all(node_weights(l + 1))
        return carry

    lax.fori_loop(1, LAYERS + 1, layer, 0)
    last_nodes(order(3))
    hand_over(order(3))

    def settle(t, carry):
        for parcel in parcels(t, True):
            parcel.wait_sent()
        for parcel in parcels(t, False):
            parcel.wait_arrived()
        return carry

    lax.fori_loop(0, NODES // TILE, settle, 0)


def processor(h_in, lat, first_edge, w_edge_in, w_edge_out, w_node_in, w_node_out):
    hbm = pl.BlockSpec(memory_space=pl.ANY)
    vmem = pl.BlockSpec(memory_space=pltpu.VMEM)
    rows = NODES * (OFFS * 2 + 8)
    return pl.pallas_call(
        functools.partial(proc_kernel, first_edge),
        in_specs=[vmem, hbm, hbm, hbm, hbm, hbm],
        out_specs=pl.BlockSpec(memory_space=pltpu.HBM),
        out_shape=jax.ShapeDtypeStruct((RING, 2, RLOC, LAT), BF16),
        scratch_shapes=[
            pltpu.VMEM((OFFS, NODES, LAT), BF16),
            pltpu.VMEM((NODES, LAT), BF16),
            pltpu.VMEM((2, NODES + 16, LAT), F32),
            pltpu.VMEM((2, NODES, LAT), F32),
            pltpu.VMEM((NODES, LAT), BF16),
            pltpu.VMEM((LAT // LANES, NODES, LANES), F32),
            pltpu.VMEM((Q, RLOC, LAT), BF16),
            pltpu.VMEM((2, 2, 8, LAT), F32),
            pltpu.VMEM((2, 3 * LAT, LAT), BF16),
            pltpu.VMEM((2, LAT, LAT), BF16),
            pltpu.VMEM((2, 2 * LAT, LAT), BF16),
            pltpu.VMEM((2, LAT, LAT), BF16),
            pltpu.SemaphoreType.DMA((2, 4)),
            pltpu.SemaphoreType.DMA((OFFS,)),
            pltpu.SemaphoreType.DMA((2,)),
            pltpu.SemaphoreType.DMA((2, 2)),
            pltpu.SemaphoreType.DMA((NODES // TILE, Q)),
            pltpu.SemaphoreType.DMA((NODES // TILE, Q)),
        ],
        compiler_params=pltpu.CompilerParams(collective_id=0, has_side_effects=True, vmem_limit_bytes=VMEM_LIMIT),
        cost_estimate=pl.CostEstimate(flops=2 * LAYERS * rows * LAT * LAT, bytes_accessed=60 * 2 ** 20, transcendentals=0),
        name="processor",
    )(h_in, lat, w_edge_in, w_edge_out, w_node_in, w_node_out)


def solution(mesh):
    ring = mesh.shape["gp"]
    row_spec = P(("dp", "gp"))
    edge_spec = P(("dp", "gp"), None, None)
    whole = P()

    def exchange(x):
        return lax.all_to_all(x, "gp", 0, 0)

    def local_run(x_prev, x_cur, forcing, grid_static, g2m_feat, m2g_feat, mesh_feat, mesh_edge_feat, norm_stats, w_grid_in, w_mesh_in, w_eemb_in, w_embed_out, w_edge_in, w_edge_out, w_node_in, w_node_out, w_grid_self, w_out_hidden, w_out_final):
        grid_dev = x_prev.shape[0]
        mesh_dev = mesh_feat.shape[0]
        half = mesh_dev // 2
        deep = 8

        def padded(x):
            return jnp.pad(x, ((0, deep - x.shape[0]), (0, 0)))

        edges = mesh_edge_feat.astype(BF16).transpose(1, 2, 0).reshape(OFFS * 4, 2, ring, RLOC).transpose(2, 0, 1, 3)
        edges = exchange(edges)
        edges = edges.reshape(ring, OFFS, 4, 2, RLOC).transpose(2, 1, 4, 0, 3).reshape(4, OFFS * RLOC, Q)
        edges = padded(jnp.roll(edges, -1, axis=2).reshape(4, OFFS * NODES))
        node_rows = mesh_feat.astype(BF16).T
        g2m_rows = g2m_feat.astype(BF16).T
        head = jnp.concatenate([node_rows[:, :half]] + [g2m_rows[:, k * half:(k + 1) * half] for k in range(RATIO)], axis=0)
        head = lax.ppermute(head, "gp", [(s, (s - 1) % ring) for s in range(ring)])
        node_rows = padded(jnp.concatenate([node_rows[:, half:], head[:3]], axis=1))
        g2m_rows = padded(jnp.concatenate([g2m_rows[:, RATIO * half:]] + [head[3 + 4 * k:7 + 4 * k] for k in range(RATIO)], axis=1))
        feats = jnp.concatenate([node_rows, g2m_rows, padded(m2g_feat.astype(BF16).T)], axis=1)
        lat = embed_static(feats, jnp.stack([padded(w_mesh_in), padded(w_eemb_in[0]), padded(w_eemb_in[1])]), w_embed_out, 1, (mesh_dev, mesh_dev + grid_dev), "embed")
        edge_lat = embed_static(edges, padded(w_eemb_in[2])[None], w_embed_out, 4, (), "embed_edges")

        w_grid = jnp.concatenate([
            jnp.pad(w_grid_in[:VARS], ((0, FEAT_CUR - VARS), (0, 0))),
            jnp.pad(w_grid_in[VARS:2 * VARS], ((0, FEAT_CUR - VARS), (0, 0))),
            padded(w_grid_in[2 * VARS:2 * VARS + 5]), padded(w_grid_in[2 * VARS + 5:])], axis=0)
        w_final = jnp.pad(w_out_final, ((0, 0), (0, LANES - VARS)))
        last = w_edge_in.shape[0] - 1
        stats = norm_stats.T
        enc_w = {"stats": stats, "w_grid": w_grid, "w_grid_out": (w_embed_out, 0), "wf": (w_edge_in, 0), "wf_out": (w_edge_out, 0), "wf_node": (w_node_in, 0), "wf_node_out": (w_node_out, 0), "w_self": w_grid_self}
        dec_w = {"stats": stats, "wl": (w_edge_in, last), "wl_out": (w_edge_out, last), "wl_node": (w_node_in, last), "wl_node_out": (w_node_out, last), "w_hidden": w_out_hidden, "w_final": w_final}
        static_rows = padded(grid_static.T)
        force = [jnp.concatenate([padded(forcing[:, s, :].T), static_rows], axis=0) for s in range(2)]

        def process(h):
            return processor(h, edge_lat, 0, w_edge_in, w_edge_out, w_node_in, w_node_out)

        now = x_cur.T
        grid_lat, h = grid_call({"cur": now, "prev": x_prev.T, "force": force[0], "g2m": lat, "mesh": lat}, enc_w, False, True, "encode")
        h = process(h)
        x_next, grid_lat, h = grid_call({"cur": now, "h_in": h, "grid_cur": grid_lat, "m2g": lat, "force": force[1], "g2m": lat, "mesh": lat}, {**dec_w, **enc_w}, True, True, "decode_encode")
        h = process(h)
        x_after, = grid_call({"cur": x_next, "h_in": h, "grid_cur": grid_lat, "m2g": lat}, dec_w, True, False, "decode")
        return x_next.T, x_after.T

    in_specs = (row_spec, row_spec, edge_spec, row_spec, row_spec, row_spec, row_spec, edge_spec, whole) + (whole,) * 11
    return jax.shard_map(local_run, mesh=mesh, in_specs=in_specs, out_specs=(row_spec, row_spec), check_vma=False)
```
